128 devices in a mesh: ep: 32 (over x, z, core), etp: 4 (over y).
Axes of the slice: x: 4, y: 4, z: 4, core: 2. Of those that a mesh axis runs over, the one named last changes fastest.
Arguments:
- tokens: bfloat16 [4096, 4096], P('ep', 'etp'), may hold values from -6 to 6
- expert_ids: int32 [4096, 8], P('ep'), may hold values from 0 to 63, all different within a row; in each aligned block of 128 rows (0 to 127, 128 to 255, ...) at most 24 rows name the same one
- gate_prob: float32 [4096, 8], P('ep'), may hold values from 0.05 to 1
- gate_weight: bfloat16 [64, 4096, 1536], P('ep', None, 'etp'), may hold values from -0.09375 to 0.09375
- up_weight: bfloat16 [64, 4096, 1536], P('ep', None, 'etp'), may hold values from -0.09375 to 0.09375
- down_weight: bfloat16 [64, 1536, 4096], P('ep', 'etp'), may hold values from -0.15625 to 0.15625
Outputs:
- mixed: bfloat16 [4096, 4096], P('ep', 'etp')
The draws below stay inside these ranges and needn't reach their ends.
Inputs may be any that keep to these rules, and one draw needn't show every extreme that they name: `expert_ids`: each row names 8 different experts. Within each aligned block of 128 rows (one token group) no expert is named more than 24 times, and in every draw some expert is named exactly 24 times in some block.
All inputs are finite; a program needn't handle non-finite values.
Results may differ from the reference program's by a relative error of at most 0.012.
Values may be sent and summed in bfloat16 or wider, within the bound.
A program may use at most 128 MiB of HBM per device.

```python
import math
import jax
import jax.numpy as jnp
import numpy as np
from jax import lax

D = 4096
FF = 1536
TOP = 8
TOK_DEV = 128
EXPERTS = 64
GROUPS = 32
TOKENS = 4096
CAP = 24
N_ETP = 4


def shard_levels(rng, shape, split, least, top_value):
    level, own = 1.0, jax.random.fold_in(rng, 6)
    for dim, shards_of in split:
        draws = jnp.exp(jax.random.uniform(jax.random.fold_in(own, dim), (shards_of,), jnp.float32, least / len(split), top_value / len(split)))
        level = level * jnp.repeat(draws, shape[dim] // shards_of).reshape([-1 if axis == dim else 1 for axis in range(len(shape))])
    return level


def assign_block(stream_key, own, number, rows, count, top, most, lean):
    ranking = jax.random.permutation(stream_key, count)
    packed, ordinary = load_shares(count, rows * top, most, lean, True), load_shares(count, rows * top, most, lean, False)
    places = jnp.arange(count)

    def named(lengths, offset_by):
        used = int((lengths > 0).sum())
        fixed = max(1, used // 4)
        moved = fixed + (places - fixed + offset_by * (used - fixed)) % max(1, count - fixed)
        return jnp.zeros((count,), jnp.int32).at[ranking[jnp.where(places < fixed, places, moved)]].set(jnp.asarray(lengths, jnp.int32))

    lengths = jnp.where(number % 4 == 0, named(packed, number // 4), named(ordinary, number - number // 4 - 1))
    mixed = jax.random.permutation(jax.random.fold_in(own, 3), count)
    source_of, sink = mixed[0:count // 2 * 2:2], mixed[1:count // 2 * 2:2]
    slack = jnp.minimum(lengths[source_of] - 1, most - lengths[sink]) // 2
    slack = jnp.where((source_of == ranking[0]) | (sink == ranking[0]) | (lengths[sink] == 0), 0, jnp.maximum(slack, 0))
    moved = jax.random.randint(jax.random.fold_in(own, 4), (count // 2,), 0, 1 << 20) % (slack + 1)
    lengths = lengths.at[source_of].add(-moved).at[sink].add(moved)
    items = jnp.searchsorted(jnp.cumsum(lengths), jnp.arange(rows * top), side="right").astype(jnp.int32)
    grid = items.reshape(top, rows).T
    grid = grid[jax.random.permutation(jax.random.fold_in(own, 1), rows)]
    offset_by = jax.random.randint(jax.random.fold_in(own, 2), (rows, 1), 0, top)
    return jnp.take_along_axis(grid, (jnp.arange(top)[None, :] + offset_by) % top, axis=1)


def load_shares(amount, total, limit, slope, full):
    weights = [(1 << 20) // math.isqrt(standing ** slope) + 1 for standing in range(1, amount + 1)]
    largest = limit if full else min(limit, max(-(-total // amount), total * weights[0] // sum(weights)))
    least = 1 if total - largest >= amount - 1 else 0
    given, rest = [largest] + [least] * (amount - 1), total - largest - least * (amount - 1)
    while rest > 0:
        free = [i for i in range(1, amount) if given[i] < largest] or [i for i in range(1, amount) if given[i] < limit]
        whole, remaining = sum([weights[i] for i in free]), rest
        for i in free:
            more = min(limit - given[i], max(1, remaining * weights[i] // whole), rest)
            given[i] = given[i] + more
            rest = rest - more
    return np.array(given)


def scatter_about(own_key, dims, spread, most, pieces=(), kind=jnp.bfloat16):
    result = jax.random.normal(own_key, dims, jnp.float32) * spread
    if len(pieces) > 0:
        result = shard_levels(own_key, dims, pieces, -0.22, 0.18) * result
    return jnp.clip(result, min=-most, max=most).astype(kind)


def setup_inputs(seed: int = 0) -> dict:
    splits = jax.random.split(jax.random.key(seed), 7)
    tokens = scatter_about(splits[0], (TOKENS, D), 1.0, 6.0, ((0, 32), (1, 4)))
    expert_ids_keys = jax.random.split(jax.random.fold_in(splits[1], 1), TOKENS // TOK_DEV)
    expert_ids_turns = jax.random.permutation(jax.random.fold_in(splits[1], 3), TOKENS // TOK_DEV)
    expert_ids = jax.vmap(lambda own, number: assign_block(jax.random.fold_in(splits[1], 2), own, number, TOK_DEV, EXPERTS, TOP, CAP, 2))(expert_ids_keys, expert_ids_turns).reshape((TOKENS, TOP))
    gate_prob = jnp.clip(0.05 + 0.95 * jax.random.uniform(splits[2], (TOKENS, TOP), jnp.float32) ** shard_levels(splits[2], (TOKENS, TOP), ((0, 32),), -0.2, 0.2), 0.05, 1.0)
    gate_weight = scatter_about(splits[3], (EXPERTS, D, FF), D ** -0.5, 0.09375, ((0, 32), (2, 4)))
    up_weight = scatter_about(splits[4], (EXPERTS, D, FF), D ** -0.5, 0.09375, ((0, 32), (2, 4)))
    down_weight = scatter_about(splits[5], (EXPERTS, FF, D), FF ** -0.5, 0.15625, ((0, 32), (1, 4)))
    return dict(tokens=tokens, expert_ids=expert_ids, gate_prob=gate_prob, gate_weight=gate_weight, up_weight=up_weight, down_weight=down_weight)


def reference(tokens, expert_ids, gate_prob, gate_weight, up_weight, down_weight):
    assigned = TOK_DEV * TOP
    grouped = expert_ids.reshape(GROUPS, assigned).astype(jnp.int32)
    onehot = (grouped[:, :, None] == jnp.arange(EXPERTS, dtype=jnp.int32)[None, None, :]).astype(jnp.int32)
    position = jnp.sum((jnp.cumsum(onehot, axis=1) - onehot) * onehot, axis=2).astype(jnp.int32)
    slot_index = (grouped * CAP + position).astype(jnp.int32)
    group_rows = jnp.arange(GROUPS, dtype=jnp.int32)[:, None]
    owners = (group_rows * TOK_DEV + (jnp.arange(assigned, dtype=jnp.int32) // TOP)[None, :]).astype(jnp.int32)
    sources = jnp.full((GROUPS, EXPERTS * CAP), TOKENS, jnp.int32).at[group_rows, slot_index].set(owners)
    scales = jnp.zeros((GROUPS, EXPERTS * CAP), jnp.float32).at[group_rows, slot_index].set(
        gate_prob.reshape(GROUPS, assigned).astype(jnp.float32))
    sources = sources.reshape(GROUPS, EXPERTS, CAP).transpose(1, 0, 2).reshape(EXPERTS, GROUPS * CAP)
    scales = scales.reshape(GROUPS, EXPERTS, CAP).transpose(1, 0, 2).reshape(EXPERTS, GROUPS * CAP)
    padded = jnp.concatenate([tokens, jnp.zeros((1, D), tokens.dtype)], axis=0)
    block = FF // N_ETP

    def expert_step(accumulated, inputs):
        w_gate, w_up, w_down, rows_from, row_scale = inputs
        expert_rows = padded[rows_from]
        gate_sum = jnp.dot(expert_rows, w_gate, preferred_element_type=jnp.float32)
        up_sum = jnp.dot(expert_rows, w_up, preferred_element_type=jnp.float32)
        hidden = (jax.nn.silu(gate_sum) * up_sum).astype(jnp.bfloat16)
        expert_out = jnp.zeros((GROUPS * CAP, D), jnp.float32)
        for part_index in range(N_ETP):
            product = jnp.dot(hidden[:, part_index * block:(part_index + 1) * block],
                              w_down[part_index * block:(part_index + 1) * block, :],
                              preferred_element_type=jnp.float32)
            rounded = lax.optimization_barrier(product.astype(jnp.bfloat16))
            expert_out = expert_out + rounded.astype(jnp.float32)
        accumulated = accumulated.at[rows_from].add(row_scale[:, None] * expert_out)
        return accumulated, None

    accumulated = jnp.zeros((TOKENS + 1, D), jnp.float32)
    accumulated, unused = lax.scan(expert_step, accumulated,
                                   (gate_weight, up_weight, down_weight, sources, scales))
    return accumulated[:TOKENS].astype(jnp.bfloat16)
```

```python
import heapq

import jax
import jax.numpy as jnp
from jax import lax
from jax.experimental import pallas as pl
from jax.experimental.pallas import tpu as pltpu
from jax.sharding import PartitionSpec as P

MESH = pl.DeviceIdType.MESH
F32 = jnp.float32
BF16 = jnp.bfloat16
X, Y, Z = 0, 1, 2
ORDERS = (
    (Y, Z, X), (X, Z, Y), (X, Y, Z),
    (Y, Z, X), (X, Z, Y), (Y, X, Z),
    (Y, Z, X), (X, Z, Y),
)
NP = len(ORDERS)
CAP = 24
PAIR = 2 * CAP


def plan():
    rate, lat = 46.6e3, 2.2
    free = {}
    arrive = {}
    done = {}
    tasks = {}

    def size(ph):
        return 16384 * 4 ** ph

    def add(name, prio, cost, after=(), needs=(), sends=()):
        tasks[name] = (prio, cost, after, needs, sends)

    for j, order in enumerate(ORDERS):
        for ph in range(3):
            a, k = order[ph], (j, ph)
            before = [("AD", j, ph - 1)] if ph else []
            s = size(ph)
            add(("AS", j, ph), (0, j, ph, 0), 0.05, before, (),
                [(a, 1, s, ("ga+",) + k), (a, -1, s, ("ga-",) + k), (a, 1, s, ("gc1",) + k), (a, -1, s, ("gc2",) + k)])
            add(("AF+", j, ph), (0, j, ph, 1), 0.05, [("AS", j, ph)], [("ga+",) + k], [(a, 1, s, ("gc3",) + k)])
            add(("AF-", j, ph), (0, j, ph, 2), 0.05, [("AS", j, ph)], [("ga-",) + k], [(a, -1, s, ("gc4",) + k)])
            add(("AD", j, ph), (0, j, ph, 3), 0.05, [("AF+", j, ph), ("AF-", j, ph)], [(f"gc{i}",) + k for i in (1, 2, 3, 4)])
        add(("LW", j), (1, j), 0.1, [("GU", j - 2)] if j >= 2 else [], [("pw", j)])
        add(("SEL", j), (3, j, 0), 0.9, [("AD", j, 2), ("ST",)] + ([("GU", j - 1)] if j else []))
        add(("GU", j), (3, j, 1), 2.2, [("SEL", j), ("LW", j)])
        add(("DW", j), (1, j), 0.1, [("CB", j - 2)] if j >= 2 else [("LW", NP - 1)], [("pd",)])
        add(("DN", j), (3, 10 + j, 1), 1.2, [("HID",), ("DW", j)] + ([("CB", j - 1)] if j else []))
        add(("CB", j), (3, 10 + j, 2), 1.0, [("DN", j)])
        for r in range(3):
            ph = 2 - r
            a, k = order[ph], (j, ph)
            s = size(ph)
            v = 0.02 + 0.15 * s / 262144
            add(("RS", j, ph), (0, 10 + j, r, 0), 0.05, [("RD", j, ph + 1)] if r else [("CB", j)], (),
                [(a, 1, s, ("ra+",) + k), (a, -1, s, ("ra-",) + k), (a, 1, s, ("rc1",) + k), (a, -1, s, ("rc2",) + k)])
            add(("RF+", j, ph), (0, 10 + j, r, 1), v, [("RS", j, ph)], [("ra+",) + k], [(a, 1, s, ("rc3",) + k)])
            add(("RF-", j, ph), (0, 10 + j, r, 2), v, [("RS", j, ph)], [("ra-",) + k], [(a, -1, s, ("rc4",) + k)])
            add(("RD", j, ph), (0, 10 + j, r, 3), 2 * v, [("RF+", j, ph), ("RF-", j, ph)], [(f"rc{i}",) + k for i in (1, 2, 3, 4)])
    add(("META",), (2, 0), 1.0, (), [("meta",)])
    for q in range(NP):
        add(("SB", q), (2, 1 + q), 0.6, [("META",)])
    add(("ST",), (2, 20), 0.0, [("SB", q) for q in range(NP)])
    add(("HID",), (3, 9), 1.5, [("GU", NP - 1)])
    arrive[("meta",)] = 5.0
    for j in range(NP):
        arrive[("pw", j)] = 4.0 + 4.5 * (j + 1)
    arrive[("pd",)] = 4.0 + 4.5 * NP + 14

    now, out = 0.0, []
    while tasks:
        ready, later = [], []
        for name, (prio, cost, after, needs, sends) in tasks.items():
            if all(d in done for d in after) and all(n in arrive for n in needs):
                t = max([0.0] + [arrive[n] for n in needs])
                if t <= now:
                    ready.append((prio, name))
                else:
                    later.append((t, prio, name))
        if not ready:
            now = min(later)[0]
            continue
        name = min(ready)[1]
        prio, cost, after, needs, sends = tasks.pop(name)
        now += cost
        for a, d, s, tag in sends:
            begin = max(now, free.get((a, d), 0.0))
            free[(a, d)] = begin + s / rate
            arrive[tag] = begin + s / rate + lat
        done[name] = now
        out.append(name)
    return out, now


SCHEDULE, PLANNED_US = plan()


def half_shape(order, ph):
    full = order[:ph]
    return (4 if X in full else 1, 4 if Z in full else 1, 64, 512 if Y in full else 128)


def kernel(tok, meta, gw, uw, dw, out, pw, pd, t_ref, w_ref, d_ref, x_ref, acc, hid, y_ref, s_ref, st_ref, ps, rk, pr, mb,
           ga, gc, gs, ra, rc, rs, tok_sem, meta_send, meta_recv, meta_own, pw_send, pw_recv, pd_send, pd_recv,
           w_sem, d_sem, *rb):
    ep = lax.axis_index("ep")
    y = lax.axis_index("etp")
    x, z, core = ep // 8, (ep // 2) % 4, ep % 2
    own = (x, y, z)

    def at(axis, delta):
        c = [x, y, z]
        c[axis] = (c[axis] + delta + 4) % 4
        return {"ep": c[X] * 8 + c[Z] * 2 + core, "etp": c[Y]}

    partner = {"ep": x * 8 + z * 2 + (1 - core), "etp": y}
    plane = [
        {"ep": ((x + dx) % 4) * 8 + ((z + dz) % 4) * 2 + core, "etp": y}
        for dx in range(4) for dz in range(4) if dx or dz
    ]

    own_tok = [
        pltpu.make_async_copy(
            tok.at[:, pl.ds(j * 128, 128)],
            t_ref.at[j, x, z, :, pl.ds(pl.multiple_of(y * 128, 128), 128)], tok_sem.at[j])
        for j in range(NP)
    ]
    for c in own_tok:
        c.start()
    g = x * 4 + z
    own_meta = pltpu.make_async_copy(meta, mb.at[g], meta_own)
    own_meta.start()

    barrier = pltpu.get_barrier_semaphore()
    greet = plane + [at(Y, 1), at(Y, -1), partner]
    for d in greet:
        pl.semaphore_signal(barrier, inc=1, device_id=d, device_id_type=MESH)
    pl.semaphore_wait(barrier, len(greet))

    def remote(src, dst, ssem, rsem, dev):
        pltpu.make_async_remote_copy(src_ref=src, dst_ref=dst, send_sem=ssem, recv_sem=rsem,
                                     device_id=dev, device_id_type=MESH).start()

    def wait(ref, sem):
        pltpu.make_async_copy(ref, ref, sem).wait()

    def slab(j, ph, pos, half=None, many=1):
        order = ORDERS[j]
        a, full = order[ph], order[:ph]

        def pick(axis):
            if axis in full:
                return pl.ds(0, 4)
            if axis == a:
                return pl.ds(pos, many)
            return pl.ds(own[axis], 1)

        cy = pick(Y)
        cols = pl.ds(0, 512) if Y in full else pl.ds(
            pl.multiple_of((pos if Y == a else y) * 128, 128), 128 * (many if Y == a else 1))
        rows = pl.ds(0, 128) if half is None else pl.ds(64 * half, 64)
        return t_ref.at[j, pick(X), pick(Z), rows, cols]

    def place(j, ph, delta):
        return (own[ORDERS[j][ph]] + delta + 4) % 4

    def run_as(j, ph):
        if ph == 0:
            own_tok[j].wait()
        a, p = ORDERS[j][ph], own[ORDERS[j][ph]]
        fwd, bwd = at(a, 1), at(a, -1)
        for half, sem_f in ((0, ga.at[j, ph, 0]), (1, gc.at[j, ph])):
            h = slab(j, ph, p, half)
            remote(h, h, gs.at[j, ph], sem_f, fwd)
            o = slab(j, ph, p, 1 - half)
            remote(o, o, gs.at[j, ph], ga.at[j, ph, 1] if half == 0 else gc.at[j, ph], bwd)

    def run_af(j, ph, sign):
        a = ORDERS[j][ph]
        half = 0 if sign > 0 else 1
        ref = slab(j, ph, place(j, ph, -sign), half)
        wait(ref, ga.at[j, ph, half])
        remote(ref, ref, gs.at[j, ph], gc.at[j, ph], at(a, sign))

    def run_ad(j, ph):
        wait(slab(j, ph, 0, None, 2), gc.at[j, ph])

    def run_lw(j):
        wait(pw.at[j], pw_recv.at[j])
        slot = j % 2
        for e, base in ((0, None), (1, pw)):
            for m, src in ((0, gw), (1, uw)):
                s = src.at[:, :, j] if base is None else pw.at[j, m]
                pltpu.make_async_copy(s, w_ref.at[slot, pl.ds(2 * e, 2), :, :, pl.ds(m * 384, 384)], w_sem.at[slot]).start()

    def run_dw(j):
        if j == 0:
            wait(pd, pd_recv)
        slot = j % 2
        for e, src in ((0, dw), (1, pd)):
            for k in range(4):
                pltpu.make_async_copy(
                    src.at[:, :, pl.ds(k * 1024 + j * 128, 128)],
                    d_ref.at[slot, pl.ds(2 * e, 2), :, pl.ds(k * 128, 128)], d_sem.at[slot]).start()

    def run_meta():
        own_meta.wait()
        wait(mb.at[pl.ds(0, 15)], meta_recv)
        ids = mb[:, 0:8, :]
        probs = mb[:, 8:16, :]
        chip = (x * 4 + z) * 4
        first = [chip + 2 * core, chip + 2 * core + 1, chip + 2 * (1 - core), chip + 2 * (1 - core) + 1]
        rows, prows = [], []
        for e in first:
            hit = ids == e.astype(F32)
            rows.append(jnp.sum(jnp.where(hit, 1.0, 0.0), axis=1))
            prows.append(jnp.sum(jnp.where(hit, probs, 0.0), axis=1))
        ind = jnp.concatenate(rows, axis=0)
        pr[...] = jnp.concatenate(prows, axis=0)
        upper = (lax.broadcasted_iota(jnp.int32, (128, 128), 0) < lax.broadcasted_iota(jnp.int32, (128, 128), 1))
        rank = jnp.dot(ind.astype(BF16), jnp.where(upper, 1.0, 0.0).astype(BF16), preferred_element_type=F32)
        odd = (lax.broadcasted_iota(jnp.int32, (64, 128), 0) % 2).astype(F32) * float(CAP)
        rk[...] = jnp.where(ind > 0.5, rank + odd, -1.0)

    def run_sb(q):
        row = lax.broadcasted_iota(jnp.int32, (PAIR, 128), 0).astype(F32)
        blocks = []
        for e in range(4):
            i = e * 16 + 2 * q
            left = jnp.where(row == rk[i:i + 1, :], 1.0, 0.0)
            right = jnp.where(row == rk[i + 1:i + 2, :], 1.0, 0.0)
            ps[e, q * PAIR:(q + 1) * PAIR, :] = jnp.sum(
                left * pr[i:i + 1, :] + right * pr[i + 1:i + 2, :], axis=1, keepdims=True)
            blocks.append(jnp.concatenate([left, right], axis=1))
        blocks.append(jnp.zeros((256 - 4 * PAIR, 256), F32))
        full = jnp.concatenate(blocks, axis=0)
        s_ref[q] = full[:4 * PAIR].astype(BF16)
        st_ref[q] = full.T.astype(BF16)
        y_ref[q, 4 * PAIR:, :] = jnp.zeros((256 - 4 * PAIR, 512), BF16)

    def run_sel(j):
        def step(i, carry):
            for k in range(4):
                q = 4 * i + k
                t = t_ref[j, 2 * i + k // 2, (k % 2) * 2:(k % 2) * 2 + 2].reshape(256, 512)
                r = jnp.dot(s_ref[q], t, preferred_element_type=F32).astype(BF16)
                for e in range(4):
                    x_ref[e, pl.ds(pl.multiple_of(q * PAIR, 16), PAIR), :] = r[e * PAIR:(e + 1) * PAIR]
            return carry

        lax.fori_loop(0, 2, step, 0)

    def run_gu(j):
        slot = j % 2
        wait(w_ref.at[slot], w_sem.at[slot])

        def step(e, carry):
            for n in range(3):
                w = w_ref[slot, e, :, :, n * 256:(n + 1) * 256].reshape(512, 256)
                r = jnp.dot(x_ref[e], w, preferred_element_type=F32)
                if j == 0:
                    acc[e, :, n * 256:(n + 1) * 256] = r
                else:
                    acc[e, :, n * 256:(n + 1) * 256] += r
            return carry

        lax.fori_loop(0, 4, step, 0)

    def run_hid():
        def step(i, carry):
            e, k = i // 8, i % 8
            rows = pl.ds(pl.multiple_of(k * 48, 16), 48)
            gate, up = acc[e, rows, 0:384], acc[e, rows, 384:768]
            h = gate / (1.0 + jnp.exp(-gate)) * up * ps[e, rows, :]
            hid[e, rows, :] = h.astype(BF16)
            return carry

        lax.fori_loop(0, 32, step, 0)

    def run_dn(j):
        slot = j % 2
        wait(d_ref.at[slot], d_sem.at[slot])

        def step(e, carry):
            r = jnp.dot(hid[e], d_ref[slot, e], preferred_element_type=F32).astype(BF16)
            for q in range(NP):
                y_ref[q, pl.ds(pl.multiple_of(e * PAIR, 16), PAIR), :] = r[q * PAIR:(q + 1) * PAIR]
            return carry

        lax.fori_loop(0, 4, step, 0)

    def run_cb(j):
        for ph in range(3):
            wait(slab(j, ph, 0, None, 3), gs.at[j, ph])

        def step(i, carry):
            for k in range(4):
                q = 4 * i + k
                r = jnp.dot(st_ref[q], y_ref[q], preferred_element_type=F32).astype(BF16)
                t_ref[j, 2 * i + k // 2, (k % 2) * 2:(k % 2) * 2 + 2] = r.reshape(2, 128, 512)
            return carry

        lax.fori_loop(0, 2, step, 0)

    def buf(j, ph):
        return rb[3 * j + ph]

    def run_rs(j, ph):
        a = ORDERS[j][ph]
        fwd, bwd = at(a, 1), at(a, -1)
        b, s = buf(j, ph), rs.at[j, ph]
        far = place(j, ph, 2)
        remote(slab(j, ph, far, 0), b.at[0], s, ra.at[j, ph, 0], fwd)
        remote(slab(j, ph, far, 1), b.at[1], s, ra.at[j, ph, 1], bwd)
        remote(slab(j, ph, place(j, ph, 1), 1), b.at[2], s, rc.at[j, ph], fwd)
        remote(slab(j, ph, place(j, ph, -1), 0), b.at[3], s, rc.at[j, ph], bwd)

    def add_into(j, ph, pos, half, parts, last=False):
        b = buf(j, ph)
        nx, nz, _, cols = half_shape(ORDERS[j], ph)
        a, full = ORDERS[j][ph], ORDERS[j][:ph]

        def index(axis, i):
            return i if axis in full else (pos if axis == a else own[axis])

        cpos = 0 if Y in full else pl.multiple_of((pos if a == Y else y) * 128, 128)
        rows = pl.ds(64 * half, 64)

        def step(i, carry):
            ix, iz = i // nz, i % nz
            spot = (j, index(X, ix), index(Z, iz), rows, pl.ds(cpos, cols))
            v = t_ref[spot].astype(F32)
            for k in parts:
                v = v + b[k, ix, iz].astype(F32)
            v = v.astype(BF16)
            if last:
                out[rows, j * 128:(j + 1) * 128] = v
            else:
                t_ref[spot] = v
            return carry

        if nx * nz == 1:
            step(0, 0)
        else:
            lax.fori_loop(0, nx * nz, step, 0)

    def run_rf(j, ph, sign):
        a, b = ORDERS[j][ph], buf(j, ph)
        half = 0 if sign > 0 else 1
        wait(b.at[half], ra.at[j, ph, half])
        pos = place(j, ph, sign)
        add_into(j, ph, pos, half, (half,))
        remote(slab(j, ph, pos, half), b.at[4 + half], rs.at[j, ph], rc.at[j, ph], at(a, sign))

    def run_rd(j, ph):
        b = buf(j, ph)
        wait(b.at[pl.ds(2, 4)], rc.at[j, ph])
        p = own[ORDERS[j][ph]]
        add_into(j, ph, p, 0, (3, 4), ph == 0)
        add_into(j, ph, p, 1, (2, 5), ph == 0)

    started = 0
    while SCHEDULE[started][0] == "AS":
        run_as(*SCHEDULE[started][1:])
        started += 1
    for d in plane:
        remote(meta, mb.at[g], meta_send, meta_recv, d)
    for j in range(NP):
        remote(gw.at[:, :, j], pw.at[j, 0], pw_send, pw_recv.at[j], partner)
        remote(uw.at[:, :, j], pw.at[j, 1], pw_send, pw_recv.at[j], partner)
    remote(dw, pd, pd_send, pd_recv, partner)

    runs = {
        "AS": run_as, "AF+": lambda j, ph: run_af(j, ph, 1), "AF-": lambda j, ph: run_af(j, ph, -1), "AD": run_ad,
        "LW": run_lw, "DW": run_dw, "SEL": run_sel, "GU": run_gu, "DN": run_dn, "CB": run_cb,
        "RS": run_rs, "RF+": lambda j, ph: run_rf(j, ph, 1), "RF-": lambda j, ph: run_rf(j, ph, -1), "RD": run_rd,
        "META": run_meta, "SB": run_sb, "ST": lambda: None, "HID": run_hid,
    }
    for task in SCHEDULE[started:]:
        runs[task[0]](*task[1:])

    for j in range(NP):
        for ph in range(3):
            wait(slab(j, ph, 0, None, 3), rs.at[j, ph])
    wait(mb.at[pl.ds(0, 15)], meta_send)
    wait(pw, pw_send)
    wait(pd, pd_send)


def body(tokens, expert_ids, gate_prob, gate_weight, up_weight, down_weight):
    meta = jnp.concatenate([expert_ids.T.astype(F32), gate_prob.T], axis=0)
    gw = gate_weight.reshape(2, 4, NP, 128, 384)
    uw = up_weight.reshape(2, 4, NP, 128, 384)
    hbm = pl.BlockSpec(memory_space=pl.ANY)
    dma = pltpu.SemaphoreType.DMA
    scratch = [
        pltpu.VMEM((NP, 4, 4, 128, 512), BF16),
        pltpu.VMEM((2, 4, 4, 128, 768), BF16),
        pltpu.VMEM((2, 4, 384, 512), BF16),
        pltpu.VMEM((4, 384, 512), BF16),
        pltpu.VMEM((4, 384, 768), F32),
        pltpu.VMEM((4, 384, 384), BF16),
        pltpu.VMEM((8, 256, 512), BF16),
        pltpu.VMEM((8, 4 * PAIR, 256), BF16),
        pltpu.VMEM((8, 256, 256), BF16),
        pltpu.VMEM((4, 384, 1), F32),
        pltpu.VMEM((64, 128), F32),
        pltpu.VMEM((64, 128), F32),
        pltpu.VMEM((16, 16, 128), F32),
        dma((NP, 3, 2)), dma((NP, 3)), dma((NP, 3)),
        dma((NP, 3, 2)), dma((NP, 3)), dma((NP, 3)),
        dma((NP,)), dma, dma, dma, dma, dma((NP,)), dma, dma, dma((2,)), dma((2,)),
    ] + [pltpu.VMEM((6,) + half_shape(order, ph), BF16) for order in ORDERS for ph in range(3)]
    return pl.pallas_call(
        kernel,
        name="moe",
        out_shape=(
            jax.ShapeDtypeStruct((128, 1024), BF16),
            jax.ShapeDtypeStruct((NP, 2, 2, 4, 128, 384), BF16),
            jax.ShapeDtypeStruct((2, 384, 4096), BF16),
        ),
        in_specs=[hbm] * 5,
        out_specs=(pl.BlockSpec(memory_space=pltpu.VMEM), hbm, hbm),
        scratch_shapes=scratch,
        compiler_params=pltpu.CompilerParams(collective_id=0, has_side_effects=True, vmem_limit_bytes=67043328),
    )(tokens, meta, gw, uw, down_weight)[0]


def solution(mesh):
    in_specs = (
        P("ep", "etp"),
        P("ep", None),
        P("ep", None),
        P("ep", None, "etp"),
        P("ep", None, "etp"),
        P("ep", "etp", None),
    )
    return jax.shard_map(body, mesh=mesh, in_specs=in_specs, out_specs=P("ep", "etp"), check_vma=False)
```

```python
import jax
import jax.numpy as jnp
from jax import lax
from jax.experimental import pallas as pl
from jax.experimental.pallas import tpu as pltpu
from jax.sharding import PartitionSpec as P

MESH = pl.DeviceIdType.MESH
F32 = jnp.float32
BF16 = jnp.bfloat16
X, Y, Z = 0, 1, 2
NP = 8
CAP = 24
PAIR = 2 * CAP
SUB = (0, -1, 1, 2)

ORDERS = (
    (Y, X, Z),
    (Z, Y, X),
    (Z, X, Y),
    (Y, X, Z),
    (X, Y, Z),
    (Z, Y, X),
    (X, Z, Y),
    (Z, X, Y),
)
BACK = (
    (Y, X, Z),
    (X, Y, Z),
    (X, Z, Y),
    (Z, Y, X),
    (Y, X, Z),
    (Z, Y, X),
    (Z, X, Y),
    (Z, X, Y),
)
THERE = ((8, 6, 1), (6, 11, 2), (0, 1, 8), (9, 9, 7), (8, 4, 13), (3, 4, 10), (5, 0, 12), (7, 8, 6))
HOME = ((23, 18, 24), (27, 21, 23), (22, 23, 17), (25, 22, 23), (28, 15, 16), (26, 19, 25), (27, 26, 14), (20, 14, 15))
FIRST = (3, 7, 4, 2, 6, 0, 1, 5)
SECOND = (0, 3, 2, 1, 4, 7, 6, 5)
BACKLOG = 3.0

COST = dict(SEL=0.76, SLOT=0.35, GU=1.9, HID=1.0, DN=1.45, CB=0.88, CBS=0.45, META=0.3, SB=0.12, ADD=0.12)


def tasks_of(orders, back):
    t = {}

    def add(name, group, cost, after=(), needs=(), sends=()):
        t[name] = (group, cost, tuple(after), tuple(needs), tuple(sends))

    def size_of(axis, ph):
        return 16384 if ph == 0 else 49152 if (ph == 2 and axis == Y) else 65536

    def phase(tag, axis, j, ph, s, per, before, second=(), up=(), down=(), last=()):
        k = (j, ph, s)
        size = size_of(axis, ph)
        v = 0.04 + per * size / 262144
        s0, s1, fp, fm = (tag + "S0",) + k, (tag + "S1",) + k, (tag + "F+",) + k, (tag + "F-",) + k
        group = (tag, j, ph, s if tag == "A" else 3 - s)
        add(s0, group + (0,), 0.04, before, (), [(axis, 1, size, ("a+", tag) + k), (axis, -1, size, ("a-", tag) + k)])
        add(s1, group + (1,), 0.04, [s0, *second], (), [(axis, 1, size, ("b+", tag) + k), (axis, -1, size, ("b-", tag) + k)])
        add(fp, group + (-1,), v, [s1, *up], [("a+", tag) + k], [(axis, 1, size, ("c+", tag) + k)])
        add(fm, group + (-1,), v, [s1, *down], [("a-", tag) + k], [(axis, -1, size, ("c-", tag) + k)])
        g = group + (-2,)
        if tag == "A" and ph == 1:
            add(("AB+",) + k, g, 0.02, [fp], [("b+", tag) + k])
            add(("AB-",) + k, g, 0.02, [fm], [("b-", tag) + k])
            add(("AD",) + k, g, 0.02, [("AB+",) + k, ("AB-",) + k], [("c+", tag) + k, ("c-", tag) + k])
        else:
            add((tag + "D",) + k, g, 2 * v if per else 0.02, [fp, fm, *last], [(n, tag) + k for n in ("b+", "b-", "c+", "c-")])

    sb = [("SB", q) for q in range(NP)]
    for j in range(NP):
        order, slot = orders[j], orders[j][2] == Y
        phase("A", order[0], j, 0, 0, 0, [])
        phase("A", order[1], j, 1, 0, 0, [("AD", j, 0, 0)])
        if slot:
            add(("SEL", j), ("SLOT", j), COST["SLOT"], [("AD", j, 1, 0)] + sb)
        for s in range(4):
            before = [("SEL", j)] if slot else [(("AD", j, 0, 0), ("AB+", j, 1, 0), ("AB-", j, 1, 0), ("AD", j, 1, 0))[s]]
            phase("A", order[2], j, 2, s, 0, before)
        here = [("AD", j, 2, s) for s in range(4)]
        if not slot:
            add(("SEL", j), ("SEL", j), COST["SEL"], here + sb)
        add(("GU", j), ("GU", j), COST["GU"], [("SEL", j)] + here, [("pw", j)])
        add(("DN", j), ("DN", j), COST["DN"], [("HID",)], [("pd",)])
        order, add_us = back[j], COST["ADD"]
        d = [("RD", j, 2, i) for i in range(4)]
        if slot:
            add(("CB", j), ("CBS", j), COST["CBS"], d)
        else:
            add(("CB", j), ("CB", j), COST["CB"], [("DN", j)])
        for s in (3, 2, 1, 0):
            phase("R", order[2], j, 2, s, add_us, [("DN" if slot else "CB", j)])
        if slot:
            phase("R", order[1], j, 1, 0, add_us, [("CB", j)])
        else:
            phase("R", order[1], j, 1, 0, add_us, [d[3]], [d[1], d[2]], [d[2]], [d[1]], [d[0]])
        phase("R", order[0], j, 0, 0, add_us, [("RD", j, 1, 0)])
    add(("META",), ("META",), COST["META"], (), [("meta",)])
    for q in range(NP):
        add(("SB", q), ("SB", q), COST["SB"], [("META",)])
    add(("HID",), ("HID",), COST["HID"], [("GU", j) for j in range(NP)])
    return t


def priority(there, home, first, second):
    def rank(g):
        if g[0] == "A":
            return (0, -9 if g[4] == -2 else there[g[1]][g[2]], g[3], g[4])
        if g[0] == "R":
            return (0, home[g[1]][g[2]], g[3], g[4])
        if g[0] == "CBS":
            return (0, home[g[1]][2], 9, 0)
        if g[0] in ("META", "SB", "SLOT"):
            return (1, 0, 0, 0)
        if g[0] in ("SEL", "GU"):
            return (2, first[g[1]], g[0] == "GU", 0)
        if g[0] == "HID":
            return (2, 50, 0, 0)
        return (2, 100 + second[g[1]], g[0] == "CB", 0)

    return rank


def plan(t, rank, backlog, trace=None):
    rate, lat = 46.6e3, 2.4
    arrive = {("meta",): 5.0, ("pd",): 54.0}
    for j in range(NP):
        arrive[("pw", j)] = 8.5 + 4.5 * j
    left = {k: len(v[2]) for k, v in t.items()}
    after = {}
    for k, v in t.items():
        for d in v[2]:
            after.setdefault(d, []).append(k)
    avail = [k for k, c in left.items() if c == 0]
    free, now, out = {}, 0.0, []
    while avail:
        best, later = None, 1e9
        for k in avail:
            group, cost, _, needs, sends = t[k]
            when = 0.0
            for n in needs:
                when = max(when, arrive.get(n, 1e9))
            if not needs:
                for a, d, _, _ in sends:
                    when = max(when, free.get((a, d), 0.0) - backlog)
            if when <= now + 1e-9:
                p = rank(group)
                if best is None or (p, k) < best:
                    best = (p, k)
            elif when < later:
                later = when
        if best is None:
            now = later
            continue
        k = best[1]
        avail.remove(k)
        _, cost, _, _, sends = t[k]
        now += cost
        for a, d, size, tag in sends:
            begin = max(now, free.get((a, d), 0.0))
            free[(a, d)] = begin + size / rate
            arrive[tag] = begin + size / rate + lat
        out.append(k)
        if trace is not None:
            trace.append((round(now, 1), k))
        for q in after.get(k, ()):
            left[q] -= 1
            if left[q] == 0:
                avail.append(q)
    return out, now


def schedule():
    trace = []
    plan(tasks_of(ORDERS, BACK), priority(THERE, HOME, FIRST, SECOND), BACKLOG, trace)
    gu = [k[1] for _, k in trace if k[0] == "GU"]
    dn = [k[1] for _, k in trace if k[0] == "DN"]
    out, early = [], [(14.0, gu[0]), (19.0, gu[1])]
    for when, k in trace:
        while early and when >= early[0][0]:
            out.append(("LW", early.pop(0)[1]))
        out.append(k)
        if k[0] == "GU":
            i = gu.index(k[1]) + 2
            out += [("LW", gu[i])] if i < NP else [("DW", dn[i - NP])]
        if k[0] == "DN" and dn.index(k[1]) + 2 < NP:
            out.append(("DW", dn[dn.index(k[1]) + 2]))
    return out, gu, dn


SCHEDULE, GU_ORDER, DN_ORDER = schedule()
SLOTTED = [j for j in range(NP) if ORDERS[j][2] == Y]
PLAIN = [j for j in range(NP) if ORDERS[j][2] != Y]


def unit(ph, s):
    return ph + s


def half_shape(j, order, ph):
    if j in SLOTTED and ph == 2:
        return (192, 128)
    full = order[:min(ph, 1)]
    return (4 if X in full else 1, 4 if Z in full else 1, 64, 512 if Y in full else 128)


def kernel(tok, meta, gw, uw, dw, out, pw, pd, t_ref, ts_ref, xs_ref, ys_ref, w_ref, d_ref, x_ref, acc, hid, y_ref,
           s_ref, st_ref, ps, rk, pr, mb, ga, gb, gc, gs, ra, rc, rs, tok_sem, meta_send, meta_recv, meta_own,
           pw_send, pw_recv, pd_send, pd_recv, w_sem, d_sem, *rb):
    ep = lax.axis_index("ep")
    y = lax.axis_index("etp")
    x, z, core = ep // 8, (ep // 2) % 4, ep % 2
    own = (x, y, z)

    def at(axis, delta):
        c = [x, y, z]
        c[axis] = (c[axis] + delta + 4) % 4
        return {"ep": c[X] * 8 + c[Z] * 2 + core, "etp": c[Y]}

    partner = {"ep": x * 8 + z * 2 + (1 - core), "etp": y}
    plane = [
        {"ep": ((x + dx) % 4) * 8 + ((z + dz) % 4) * 2 + core, "etp": y}
        for dx in range(4) for dz in range(4) if dx or dz
    ]

    def lanes(i, n=1):
        return pl.ds(pl.multiple_of(i * 128, 128), 128 * n)

    own_tok = []
    for j in range(NP):
        dst = ts_ref.at[SLOTTED.index(j), x, z] if j in SLOTTED else t_ref.at[PLAIN.index(j), x, z, :, lanes(y)]
        own_tok.append(pltpu.make_async_copy(tok.at[:, pl.ds(j * 128, 128)], dst, tok_sem.at[j]))
    for c in own_tok:
        c.start()
    g = x * 4 + z
    own_meta = pltpu.make_async_copy(meta, mb.at[g], meta_own)
    own_meta.start()

    barrier = pltpu.get_barrier_semaphore()
    greet = plane + [at(Y, 1), at(Y, -1), partner]
    for d in greet:
        pl.semaphore_signal(barrier, inc=1, device_id=d, device_id_type=MESH)
    pl.semaphore_wait(barrier, len(greet))

    def remote(src, dst, ssem, rsem, dev):
        pltpu.make_async_remote_copy(src_ref=src, dst_ref=dst, send_sem=ssem, recv_sem=rsem,
                                     device_id=dev, device_id_type=MESH).start()

    def wait(ref, sem):
        pltpu.make_async_copy(ref, ref, sem).wait()

    def place(axis, delta):
        return (own[axis] + delta + 4) % 4

    def spot(order, ph, pos, sub):
        p = list(own)
        if ph >= 1:
            p[order[0]] = None
        if ph == 2:
            p[order[1]] = place(order[1], SUB[sub])
        p[order[ph]] = pos
        return p

    def slab(order, j, ph, sub, pos, half=None, many=1):
        if j in SLOTTED and ph == 2:
            rows = pl.ds(0, 384) if half is None else pl.ds(192 * half, 192)
            return xs_ref.at[SLOTTED.index(j), sub, rows, lanes(pos, many)]
        p, a = spot(order, ph, pos, sub), order[ph]
        rows = pl.ds(0, 128) if half is None else pl.ds(64 * half, 64)
        ix, iz = (pl.ds(0, 4) if p[i] is None else pl.ds(p[i], many if i == a else 1) for i in (X, Z))
        if j in SLOTTED:
            return ts_ref.at[SLOTTED.index(j), ix, iz, rows, :]
        cols = pl.ds(0, 512) if p[Y] is None else lanes(p[Y], many if a == Y else 1)
        return t_ref.at[PLAIN.index(j), ix, iz, rows, cols]

    def run_as(j, ph, s, first):
        if ph == 0 and first:
            own_tok[j].wait()
        o = ORDERS[j]
        a, u = o[ph], unit(ph, s)
        p = own[a]
        for half, sign in ((0, 1), (1, -1)) if first else ((1, 1), (0, -1)):
            if first:
                sem = ga.at[j, u, half]
            elif ph == 1:
                sem = gb.at[j, half]
            else:
                sem = gc.at[j, u]
            h = slab(o, j, ph, s, p, half)
            remote(h, h, gs.at[j, u], sem, at(a, sign))

    def run_af(j, ph, s, sign):
        o, u = ORDERS[j], unit(ph, s)
        half = 0 if sign > 0 else 1
        ref = slab(o, j, ph, s, place(o[ph], -sign), half)
        wait(ref, ga.at[j, u, half])
        remote(ref, ref, gs.at[j, u], gc.at[j, u], at(o[ph], sign))

    def run_ab(j, ph, s, sign):
        half = 1 if sign > 0 else 0
        wait(slab(ORDERS[j], j, ph, s, place(ORDERS[j][ph], -sign), half), gb.at[j, half])

    def run_ad(j, ph, s):
        wait(slab(ORDERS[j], j, ph, s, 0, None, 1 if ph == 1 else 2), gc.at[j, unit(ph, s)])

    def run_lw(j):
        wait(pw.at[j], pw_recv.at[j])
        slot = GU_ORDER.index(j) % 2
        for e in range(2):
            for m, src in ((0, gw), (1, uw)):
                s = pw.at[j, m] if e else src.at[:, :, j]
                pltpu.make_async_copy(s, w_ref.at[slot, pl.ds(2 * e, 2), :, :, pl.ds(m * 384, 384)], w_sem.at[slot]).start()

    def run_dw(j):
        if j == DN_ORDER[0]:
            wait(pd, pd_recv)
        slot = DN_ORDER.index(j) % 2
        for e, src in ((0, dw), (1, pd)):
            for k in range(4):
                pltpu.make_async_copy(
                    src.at[:, :, pl.ds(k * 1024 + j * 128, 128)],
                    d_ref.at[slot, pl.ds(2 * e, 2), :, pl.ds(k * 128, 128)], d_sem.at[slot]).start()

    def run_meta():
        own_meta.wait()
        wait(mb.at[pl.ds(0, 15)], meta_recv)
        ids = mb[:, 0:8, :]
        probs = mb[:, 8:16, :]
        chip = (x * 4 + z) * 4
        rows, prows = [], []
        for e in (chip + 2 * core, chip + 2 * core + 1, chip + 2 * (1 - core), chip + 2 * (1 - core) + 1):
            hit = ids == e.astype(F32)
            rows.append(jnp.sum(jnp.where(hit, 1.0, 0.0), axis=1))
            prows.append(jnp.sum(jnp.where(hit, probs, 0.0), axis=1))
        ind = jnp.concatenate(rows, axis=0)
        pr[...] = jnp.concatenate(prows, axis=0)
        upper = (lax.broadcasted_iota(jnp.int32, (128, 128), 0) < lax.broadcasted_iota(jnp.int32, (128, 128), 1))
        rank = jnp.dot(ind.astype(BF16), jnp.where(upper, 1.0, 0.0).astype(BF16), preferred_element_type=F32)
        odd = (lax.broadcasted_iota(jnp.int32, (64, 128), 0) % 2).astype(F32) * float(CAP)
        rk[...] = jnp.where(ind > 0.5, rank + odd, -1.0)

    def run_sb(q):
        row = lax.broadcasted_iota(jnp.int32, (PAIR, 128), 0).astype(F32)
        blocks = []
        for e in range(4):
            i = e * 16 + 2 * q
            left = jnp.where(row == rk[i:i + 1, :], 1.0, 0.0)
            right = jnp.where(row == rk[i + 1:i + 2, :], 1.0, 0.0)
            weight = jnp.sum(left * pr[i:i + 1, :] + right * pr[i + 1:i + 2, :], axis=1, keepdims=True)
            ps[e, q * PAIR:(q + 1) * PAIR, :] = jnp.broadcast_to(0.5 * weight, (PAIR, 128))
            blocks.append(jnp.concatenate([left, right], axis=1))
        blocks.append(jnp.zeros((256 - 4 * PAIR, 256), F32))
        full = jnp.concatenate(blocks, axis=0)
        s_ref[q] = full[:4 * PAIR].astype(BF16)
        st_ref[q] = full.T.astype(BF16)
        y_ref[q, 4 * PAIR:, :] = jnp.zeros((256 - 4 * PAIR, 512), BF16)
        for i in range(len(SLOTTED)):
            ys_ref[i, q, 4 * PAIR:, :] = jnp.zeros((256 - 4 * PAIR, 128), BF16)

    def run_sel(j):
        slotted = j in SLOTTED

        def step(i, carry):
            for k in range(4):
                q = 4 * i + k
                gx, gz = 2 * i + k // 2, slice((k % 2) * 2, (k % 2) * 2 + 2)
                if slotted:
                    t = ts_ref[SLOTTED.index(j), gx, gz].reshape(256, 128)
                else:
                    t = t_ref[PLAIN.index(j), gx, gz].reshape(256, 512)
                r = jnp.dot(s_ref[q], t, preferred_element_type=F32).astype(BF16)
                for e in range(4):
                    rows = pl.ds(pl.multiple_of(q * PAIR, 16), PAIR)
                    if slotted:
                        xs_ref[SLOTTED.index(j), e, rows, lanes(y)] = r[e * PAIR:(e + 1) * PAIR]
                    else:
                        x_ref[e, rows, :] = r[e * PAIR:(e + 1) * PAIR]
            return carry

        lax.fori_loop(0, 2, step, 0)

    def run_gu(j):
        slot = GU_ORDER.index(j) % 2
        wait(w_ref.at[slot], w_sem.at[slot])

        def step(e, carry):
            rows = xs_ref[SLOTTED.index(j), e] if j in SLOTTED else x_ref[e]
            for n in range(3):
                w = w_ref[slot, e, :, :, n * 256:(n + 1) * 256].reshape(512, 256)
                r = jnp.dot(rows, w, preferred_element_type=F32)
                if j == GU_ORDER[0]:
                    acc[e, :, n * 256:(n + 1) * 256] = r
                else:
                    acc[e, :, n * 256:(n + 1) * 256] += r
            return carry

        lax.fori_loop(0, 4, step, 0)

    def run_hid():
        def step(i, carry):
            e, k = i // 4, i % 4
            rows = pl.ds(pl.multiple_of(k * 96, 16), 96)
            w = ps[e, rows, :]
            for n in range(3):
                gate, up = acc[e, rows, n * 128:(n + 1) * 128], acc[e, rows, 384 + n * 128:384 + (n + 1) * 128]
                h = (gate * up * w) * (1.0 + jnp.tanh(0.5 * gate))
                hid[e, rows, n * 128:(n + 1) * 128] = h.astype(BF16)
            return carry

        lax.fori_loop(0, 16, step, 0)

    def run_dn(j):
        slot = DN_ORDER.index(j) % 2
        wait(d_ref.at[slot], d_sem.at[slot])
        slotted = j in SLOTTED
        if slotted:
            for s in range(4):
                wait(slab(ORDERS[j], j, 2, s, 0, None, 3), gs.at[j, unit(2, s)])

        def step(e, carry):
            r = jnp.dot(hid[e], d_ref[slot, e], preferred_element_type=F32).astype(BF16)
            if slotted:
                xs_ref[SLOTTED.index(j), e] = r
            else:
                for q in range(NP):
                    y_ref[q, pl.ds(pl.multiple_of(e * PAIR, 16), PAIR), :] = r[q * PAIR:(q + 1) * PAIR]
            return carry

        lax.fori_loop(0, 4, step, 0)

    def run_cb(j):
        slotted = j in SLOTTED
        for ph, s in ((0, 0), (1, 0)) + (() if slotted else tuple((2, s) for s in range(4))):
            wait(slab(ORDERS[j], j, ph, s, 0, None, 3), gs.at[j, unit(ph, s)])

        def step(i, carry):
            for k in range(4):
                q = 4 * i + k
                gx, gz = 2 * i + k // 2, slice((k % 2) * 2, (k % 2) * 2 + 2)
                rows = ys_ref[SLOTTED.index(j), q] if slotted else y_ref[q]
                r = jnp.dot(st_ref[q], rows, preferred_element_type=F32).astype(BF16)
                if slotted:
                    ts_ref[SLOTTED.index(j), gx, gz] = r.reshape(2, 128, 128)
                else:
                    t_ref[PLAIN.index(j), gx, gz] = r.reshape(2, 128, 512)
            return carry

        lax.fori_loop(0, 2, step, 0)

    def buf(j, ph, s):
        return rb[3 * j + ph].at[s]

    def run_rs(j, ph, s, first):
        o = BACK[j]
        a, u = o[ph], unit(ph, s)
        b = buf(j, ph, s)
        for half, sign in ((0, 1), (1, -1)) if first else ((1, 1), (0, -1)):
            pos = place(a, 2 if first else sign)
            sem = ra.at[j, u, half] if first else rc.at[j, u]
            remote(slab(o, j, ph, s, pos, half), b.at[half if first else 3 - half], rs.at[j, u], sem, at(a, sign))

    def add_into(j, ph, s, pos, half, parts, final):
        b, o = rb[3 * j + ph], BACK[j]
        if j in SLOTTED and ph == 2:
            i = SLOTTED.index(j)
            v = xs_ref[i, s, pl.ds(192 * half, 192), lanes(pos)].astype(F32)
            for k in parts:
                v = v + b[s, k].astype(F32)
            v = v.astype(BF16)
            if final:
                for q in range(4):
                    ys_ref[i, 4 * half + q, s * PAIR:(s + 1) * PAIR, :] = v[q * PAIR:(q + 1) * PAIR]
            else:
                xs_ref[i, s, pl.ds(192 * half, 192), lanes(pos)] = v
            return
        nx, nz, _, cols = half_shape(j, o, ph)
        p = spot(o, ph, pos, s)
        rows = pl.ds(64 * half, 64)

        def step(i, carry):
            ix, iz = i // nz, i % nz
            gx, gz = ix if p[X] is None else p[X], iz if p[Z] is None else p[Z]
            if j in SLOTTED:
                ref, where = ts_ref, (SLOTTED.index(j), gx, gz, rows, slice(None))
            else:
                ref = t_ref
                where = (PLAIN.index(j), gx, gz, rows, slice(None) if p[Y] is None else lanes(p[Y]))
            v = ref[where].astype(F32)
            for k in parts:
                v = v + b[s, k, ix, iz].astype(F32)
            v = v.astype(BF16)
            if final and ph == 0:
                out[rows, j * 128:(j + 1) * 128] = v
            else:
                ref[where] = v
            return carry

        if nx * nz == 1:
            step(0, 0)
        else:
            lax.fori_loop(0, nx * nz, step, 0)

    def run_rf(j, ph, s, sign):
        o, u, b = BACK[j], unit(ph, s), buf(j, ph, s)
        half = 0 if sign > 0 else 1
        wait(b.at[half], ra.at[j, u, half])
        pos = place(o[ph], sign)
        add_into(j, ph, s, pos, half, (half,), False)
        remote(slab(o, j, ph, s, pos, half), b.at[4 + half], rs.at[j, u], rc.at[j, u], at(o[ph], sign))

    def run_rd(j, ph, s):
        wait(buf(j, ph, s).at[pl.ds(2, 4)], rc.at[j, unit(ph, s)])
        p = own[BACK[j][ph]]
        add_into(j, ph, s, p, 0, (3, 4), True)
        add_into(j, ph, s, p, 1, (2, 5), True)

    started = 0
    while SCHEDULE[started][0] in ("AS0", "AS1"):
        k = SCHEDULE[started]
        run_as(*k[1:], k[0] == "AS0")
        started += 1
    for d in plane:
        remote(meta, mb.at[g], meta_send, meta_recv, d)
    for j in GU_ORDER:
        remote(gw.at[:, :, j], pw.at[j, 0], pw_send, pw_recv.at[j], partner)
        remote(uw.at[:, :, j], pw.at[j, 1], pw_send, pw_recv.at[j], partner)
    remote(dw, pd, pd_send, pd_recv, partner)

    runs = {
        "AS0": lambda *k: run_as(*k, True), "AS1": lambda *k: run_as(*k, False),
        "AF+": lambda *k: run_af(*k, 1), "AF-": lambda *k: run_af(*k, -1),
        "AB+": lambda *k: run_ab(*k, 1), "AB-": lambda *k: run_ab(*k, -1), "AD": run_ad,
        "LW": run_lw, "DW": run_dw, "SEL": run_sel, "GU": run_gu, "DN": run_dn, "CB": run_cb,
        "RS0": lambda *k: run_rs(*k, True), "RS1": lambda *k: run_rs(*k, False),
        "RF+": lambda *k: run_rf(*k, 1), "RF-": lambda *k: run_rf(*k, -1), "RD": run_rd,
        "META": run_meta, "SB": run_sb, "HID": run_hid,
    }
    for task in SCHEDULE[started:]:
        runs[task[0]](*task[1:])

    for j in range(NP):
        for ph in range(3):
            for s in range(4 if ph == 2 else 1):
                wait(slab(BACK[j], j, ph, s, 0, None, 3), rs.at[j, unit(ph, s)])
    wait(mb.at[pl.ds(0, 15)], meta_send)
    wait(pw, pw_send)
    wait(pd, pd_send)


def body(tokens, expert_ids, gate_prob, gate_weight, up_weight, down_weight):
    meta = jnp.concatenate([expert_ids.T.astype(F32), gate_prob.T], axis=0)
    gw = gate_weight.reshape(2, 4, NP, 128, 384)
    uw = up_weight.reshape(2, 4, NP, 128, 384)
    hbm = pl.BlockSpec(memory_space=pl.ANY)
    dma = pltpu.SemaphoreType.DMA
    ns = len(SLOTTED)
    scratch = [
        pltpu.VMEM((NP - ns, 4, 4, 128, 512), BF16),
        pltpu.VMEM((ns, 4, 4, 128, 128), BF16),
        pltpu.VMEM((ns, 4, 384, 512), BF16),
        pltpu.VMEM((ns, 8, 256, 128), BF16),
        pltpu.VMEM((2, 4, 4, 128, 768), BF16),
        pltpu.VMEM((2, 4, 384, 512), BF16),
        pltpu.VMEM((4, 384, 512), BF16),
        pltpu.VMEM((4, 384, 768), F32),
        pltpu.VMEM((4, 384, 384), BF16),
        pltpu.VMEM((8, 256, 512), BF16),
        pltpu.VMEM((8, 4 * PAIR, 256), BF16),
        pltpu.VMEM((8, 256, 256), BF16),
        pltpu.VMEM((4, 384, 128), F32),
        pltpu.VMEM((64, 128), F32),
        pltpu.VMEM((64, 128), F32),
        pltpu.VMEM((16, 16, 128), F32),
        dma((NP, 6, 2)), dma((NP, 2)), dma((NP, 6)), dma((NP, 6)),
        dma((NP, 6, 2)), dma((NP, 6)), dma((NP, 6)),
        dma((NP,)), dma, dma, dma, dma, dma((NP,)), dma, dma, dma((2,)), dma((2,)),
    ] + [
        pltpu.VMEM((4 if ph == 2 else 1, 6) + half_shape(j, BACK[j], ph), BF16)
        for j in range(NP) for ph in range(3)
    ]
    return pl.pallas_call(
        kernel,
        name="moe",
        out_shape=(
            jax.ShapeDtypeStruct((128, 1024), BF16),
            jax.ShapeDtypeStruct((NP, 2, 2, 4, 128, 384), BF16),
            jax.ShapeDtypeStruct((2, 384, 4096), BF16),
        ),
        in_specs=[hbm] * 5,
        out_specs=(pl.BlockSpec(memory_space=pltpu.VMEM), hbm, hbm),
        scratch_shapes=scratch,
        compiler_params=pltpu.CompilerParams(collective_id=0, has_side_effects=True, vmem_limit_bytes=67043328),
    )(tokens, meta, gw, uw, down_weight)[0]


def solution(mesh):
    in_specs = (
        P("ep", "etp"),
        P("ep", None),
        P("ep", None),
        P("ep", None, "etp"),
        P("ep", None, "etp"),
        P("ep", "etp", None),
    )
    return jax.shard_map(body, mesh=mesh, in_specs=in_specs, out_specs=P("ep", "etp"), check_vma=False)
```

```python
import jax
import jax.numpy as jnp
from jax import lax
from jax.experimental import pallas as pl
from jax.experimental.pallas import tpu as pltpu
from jax.sharding import PartitionSpec as P

MESH = pl.DeviceIdType.MESH
F32 = jnp.float32
BF16 = jnp.bfloat16
X, Y, Z = 0, 1, 2
NP = 8
CAP = 24
PAIR = 2 * CAP
SUB = (0, -1, 1, 2)

ORDERS = (
    (Z, Y, X),
    (Z, X, Y),
    (X, Y, Z),
    (Z, X, Y),
    (Y, X, Z),
    (Z, Y, X),
    (Z, X, Y),
    (X, Y, Z),
)
BACK = (
    (X, Y, Z),
    (Z, X, Y),
    (X, Y, Z),
    (Z, X, Y),
    (Y, X, Z),
    (Z, Y, X),
    (Z, X, Y),
    (Z, Y, X),
)
THERE = ((2, 9, 11), (5, 2, 0), (10, 4, 2), (10, 3, 2), (10, 8, 2), (2, 3, 12), (10, 11, 3), (1, 9, 6))
HOME = ((3, 11, 11), (9, 4, 10), (5, 11, 7), (10, 3, 10), (1, 8, 11), (13, 11, 1), (7, 11, 10), (13, 11, 7))
FIRST = (0, 1, 2, 3, 4, 5, 6, 7)
SECOND = (2, 6, 5, 4, 7, 1, 3, 0)
BACKLOG = 2.0

SPLIT = (1, 4, 4)
COST = dict(SEL=0.76, SLOT=0.35, GU=1.9, HID=1.0, DN=1.45, CB=0.88, CBS=0.45, META=0.3, SB=0.12, ADD=0.12)


def tasks_of(orders, back, first, second):
    t = {}

    def add(name, group, cost, after=(), needs=(), sends=()):
        t[name] = (group, cost, tuple(after), tuple(needs), tuple(sends))

    def size_of(axis, ph):
        return 16384 if ph < 2 else 49152 if axis == Y else 65536

    def phase(tag, axis, j, ph, s, per, before, second=(), up=(), down=(), last=()):
        k = (j, ph, s)
        size = size_of(axis, ph)
        v = 0.04 + per * size / 262144
        s0, s1, fp, fm = (tag + "S0",) + k, (tag + "S1",) + k, (tag + "F+",) + k, (tag + "F-",) + k
        group = (tag, j, ph, s if tag == "A" else 3 - s)
        add(s0, group + (0,), 0.04, before, (), [(axis, 1, size, ("a+", tag) + k), (axis, -1, size, ("a-", tag) + k)])
        add(s1, group + (1,), 0.04, [s0, *second], (), [(axis, 1, size, ("b+", tag) + k), (axis, -1, size, ("b-", tag) + k)])
        add(fp, group + (-1,), v, [s1, *up], [("a+", tag) + k], [(axis, 1, size, ("c+", tag) + k)])
        add(fm, group + (-1,), v, [s1, *down], [("a-", tag) + k], [(axis, -1, size, ("c-", tag) + k)])
        g = group + (-2,)
        if tag == "A" and ph < 2:
            add(("AB+",) + k, g, 0.02, [fp], [("b+", tag) + k])
            add(("AB-",) + k, g, 0.02, [fm], [("b-", tag) + k])
            add(("AD",) + k, g, 0.02, [("AB+",) + k, ("AB-",) + k], [("c+", tag) + k, ("c-", tag) + k])
        else:
            add((tag + "D",) + k, g, 2 * v if per else 0.02, [fp, fm, *last], [(n, tag) + k for n in ("b+", "b-", "c+", "c-")])

    def every(kind, j, ph):
        return [(kind, j, ph, s) for s in range(SPLIT[ph])]

    def parts(split):
        return range(4) if split else (None,)

    def share(kind, e):
        return COST[kind] if e is None else COST[kind] / 4

    def gu_end(j):
        return ("GU", j, 3 if j == first[-1] else None)

    def dn_end(j):
        return ("DN", j, 3 if second.index(j) < 2 else None)

    sb = [("SB", q) for q in range(NP)]
    plain = [j for j in first if orders[j][2] != Y]
    back_plain = [j for j in second if orders[j][2] != Y]
    for j in range(NP):
        order, slot = orders[j], orders[j][2] == Y
        for ph in range(3):
            for s in range(SPLIT[ph]):
                if ph == 0:
                    before = []
                elif ph == 2 and slot:
                    before = [("SEL", j)]
                elif ph == 2 and s == 0:
                    before = every("AD", j, 0)
                elif SPLIT[ph] == 1:
                    before = every("AD", j, ph - 1)
                else:
                    before = ([], every("AB+", j, ph - 1), every("AB-", j, ph - 1), every("AD", j, ph - 1))[s]
                phase("A", order[ph], j, ph, s, 0, before)
        at = first.index(j)
        turn = [gu_end(first[at - 1])] if at else []
        if slot:
            add(("SEL", j), ("SLOT", j), COST["SLOT"], every("AD", j, 1) + sb)
        else:
            i = plain.index(j)
            add(("SEL", j), ("SEL", j), COST["SEL"], every("AD", j, 2) + sb + ([gu_end(plain[i - 2])] if i > 1 else []))
        for e in parts(j == first[-1]):
            here = every("AD", j, 2) if e is None else [("AD", j, 2, e)]
            prev = [("GU", j, e - 1)] if e else turn
            add(("GU", j, e), ("GU", j, e or 0), share("GU", e), [("SEL", j)] + (here if slot else []) + prev, [("pw", at)])
        at = second.index(j)
        i = 0 if slot else back_plain.index(j)
        for e in parts(at < 2):
            prev = [("DN", j, e - 1)] if e else []
            if at == 1:
                prev.append(("DN", second[0], e))
            if at > 1:
                prev += [dn_end(second[at - 1]), dn_end(second[at - 2])]
            if not slot and i > 1:
                prev.append(("CB", back_plain[i - 2]))
            add(("DN", j, e), ("DN", j, e or 0), share("DN", e), [("HID", 3 if e is None else e)] + prev, [("pd",)])
        order, add_us = back[j], COST["ADD"]
        if slot:
            add(("CB", j), ("CBS", j), COST["CBS"], every("RD", j, 2))
        else:
            add(("CB", j), ("CB", j), COST["CB"], [dn_end(j)])
        for ph in (2, 1, 0):
            for s in range(SPLIT[ph] - 1, -1, -1):
                if ph == 2:
                    phase("R", order[2], j, 2, s, add_us, [(("DN", j, s) if at < 2 else dn_end(j)) if slot else ("CB", j)])
                elif ph == 1 and slot:
                    phase("R", order[1], j, 1, s, add_us, [("CB", j)])
                elif SPLIT[ph + 1] == 1:
                    phase("R", order[ph], j, ph, s, add_us, [("RD", j, ph + 1, 0)])
                else:
                    d = [[("RD", j, ph + 1, i)] for i in range(4)]
                    phase("R", order[ph], j, ph, s, add_us, d[3], d[1] + d[2], d[2], d[1], d[0])
    add(("MA",), ("M",), 0.05, (), (), [(X, 1, 8192, ("m0",)), (X, -1, 8192, ("m1",))])
    add(("MB",), ("M",), 0.05, [("MA",)], [("m0",), ("m1",)], [(X, 1, 8192, ("m2",))])
    add(("MC",), ("M",), 0.05, [("MB",)], [("m2",)], [(Z, 1, 32768, ("m3",)), (Z, -1, 32768, ("m4",))])
    add(("MD",), ("M",), 0.05, [("MC",)], [("m3",), ("m4",)], [(Z, 1, 32768, ("m5",))])
    add(("META",), ("META",), COST["META"], [("MD",)], [("m5",)])
    for q in range(NP):
        add(("SB", q), ("SB", q), COST["SB"], [("META",)])
    for e in range(4):
        add(("HID", e), ("HID", e), COST["HID"] / 4, [("GU", first[NP - 1], e)])
    return t


def priority(there, home, first, second):
    def rank(g):
        if g[0] == "A":
            return (0, -9 if g[4] == -2 else there[g[1]][g[2]], g[3], g[4])
        if g[0] == "R":
            return (0, home[g[1]][g[2]], g[3], g[4])
        if g[0] == "CBS":
            return (0, home[g[1]][2], 9, 0)
        if g[0] == "M":
            return (0, -8, 0, 0)
        if g[0] in ("META", "SB", "SLOT"):
            return (1, 0, 0, 0)
        if g[0] in ("SEL", "GU"):
            return (2, first.index(g[1]), g[0] == "GU", 0)
        if g[0] == "HID":
            return (2, 50, 0, 0)
        if g[0] == "CB":
            return (2, 51, 0, 0)
        return (2, 100 + second.index(g[1]), 0, g[2])

    return rank


def plan(t, rank, backlog, trace=None):
    rate, lat = 46.6e3, 2.4
    arrive = {("pd",): 54.0}
    for j in range(NP):
        arrive[("pw", j)] = 8.5 + 4.5 * j
    ids = {k: i for i, k in enumerate(sorted(t, key=lambda k: tuple(str(v) for v in k)))}
    left = {k: len(v[2]) for k, v in t.items()}
    after = {}
    for k, v in t.items():
        for d in v[2]:
            after.setdefault(d, []).append(k)
    avail = [k for k, c in left.items() if c == 0]
    free, now, out = {}, 0.0, []
    while avail:
        best, later = None, 1e9
        for k in avail:
            group, cost, _, needs, sends = t[k]
            when = 0.0
            for n in needs:
                when = max(when, arrive.get(n, 1e9))
            if not needs:
                for a, d, _, _ in sends:
                    when = max(when, free.get((a, d), 0.0) - backlog)
            if when <= now + 1e-9:
                p = rank(group)
                if best is None or (p, ids[k]) < best[:2]:
                    best = (p, ids[k], k)
            elif when < later:
                later = when
        if best is None:
            now = later
            continue
        k = best[2]
        avail.remove(k)
        _, cost, _, _, sends = t[k]
        now += cost
        for a, d, size, tag in sends:
            begin = max(now, free.get((a, d), 0.0))
            free[(a, d)] = begin + size / rate
            arrive[tag] = begin + size / rate + lat
        out.append(k)
        if trace is not None:
            trace.append((round(now, 1), k))
        for q in after.get(k, ()):
            left[q] -= 1
            if left[q] == 0:
                avail.append(q)
    return out, now


def schedule():
    trace = []
    plan(tasks_of(ORDERS, BACK, FIRST, SECOND), priority(THERE, HOME, FIRST, SECOND), BACKLOG, trace)
    out, early = [], [(14.0, FIRST[0]), (19.0, FIRST[1])]
    for when, k in trace:
        while early and when >= early[0][0]:
            out.append(("LW", early.pop(0)[1]))
        out.append(k)
        if k[0] == "GU" and k[2] in (None, 3):
            i = FIRST.index(k[1]) + 2
            out += [("LW", FIRST[i])] if i < NP else [("DW", SECOND[i - NP])]
        if k[0] == "DN" and k[2] in (None, 3) and SECOND.index(k[1]) + 2 < NP:
            out.append(("DW", SECOND[SECOND.index(k[1]) + 2]))
    return out


SCHEDULE = schedule()
SLOTTED = [j for j in range(NP) if ORDERS[j][2] == Y]
PLAIN = [j for j in range(NP) if ORDERS[j][2] != Y]
PLAIN_TURN = {j: i % 2 for i, j in enumerate(k for k in FIRST if k in PLAIN)}
BACK_PLAIN = [j for j in SECOND if ORDERS[j][2] != Y]


def unit(ph, s):
    return sum(SPLIT[:ph]) + s


def half_shape(j, order, ph):
    if j in SLOTTED and ph == 2:
        return (192, 128)
    full = order[:1] if ph == 2 else ()
    return (4 if X in full else 1, 4 if Z in full else 1, 64, 512 if Y in full else 128)


def kernel(tok, ids_t, prob_t, gw, uw, dw, out, pw, pd, t_ref, ts_ref, xs_ref, ys_ref, w_ref, d_ref, x_ref, acc, hid, y_ref,
           s_ref, st_ref, ps, rk, pr, mbi, mbp, ga, gb, gc, gs, ra, rc, rs, tok_sem, meta_send, meta_recv, meta_own,
           pw_send, pw_recv, pd_send, pd_recv, w_sem, d_sem, *rb):
    ep = lax.axis_index("ep")
    y = lax.axis_index("etp")
    x, z, core = ep // 8, (ep // 2) % 4, ep % 2
    own = (x, y, z)

    def at(axis, delta):
        c = [x, y, z]
        c[axis] = (c[axis] + delta + 4) % 4
        return {"ep": c[X] * 8 + c[Z] * 2 + core, "etp": c[Y]}

    partner = {"ep": x * 8 + z * 2 + (1 - core), "etp": y}
    def lanes(i, n=1):
        return pl.ds(pl.multiple_of(i * 128, 128), 128 * n)

    own_tok = []
    for j in range(NP):
        dst = ts_ref.at[SLOTTED.index(j), x, z] if j in SLOTTED else t_ref.at[PLAIN.index(j), x, z, :, lanes(y)]
        own_tok.append(pltpu.make_async_copy(tok.at[:, pl.ds(j * 128, 128)], dst, tok_sem.at[j]))
    for c in own_tok:
        c.start()
    tables = ((ids_t, mbi), (prob_t, mbp))
    own_meta = [pltpu.make_async_copy(src, dst.at[x, z], meta_own.at[i]) for i, (src, dst) in enumerate(tables)]
    for c in own_meta:
        c.start()

    barrier = pltpu.get_barrier_semaphore()
    greet = [at(a, d) for a in (X, Y, Z) for d in (1, -1)] + [partner]
    for d in greet:
        pl.semaphore_signal(barrier, inc=1, device_id=d, device_id_type=MESH)
    pl.semaphore_wait(barrier, len(greet))

    def remote(src, dst, ssem, rsem, dev):
        pltpu.make_async_remote_copy(src_ref=src, dst_ref=dst, send_sem=ssem, recv_sem=rsem,
                                     device_id=dev, device_id_type=MESH).start()

    def wait(ref, sem):
        pltpu.make_async_copy(ref, ref, sem).wait()

    def place(axis, delta):
        return (own[axis] + delta + 4) % 4

    def spot(order, ph, pos, sub):
        p = list(own)
        if ph == 1:
            p[order[0]] = place(order[0], SUB[sub])
        if ph == 2:
            p[order[0]] = None
            p[order[1]] = place(order[1], SUB[sub])
        p[order[ph]] = pos
        return p

    def slab(order, j, ph, sub, pos, half=None, many=1):
        if j in SLOTTED and ph == 2:
            rows = pl.ds(0, 384) if half is None else pl.ds(192 * half, 192)
            return xs_ref.at[SLOTTED.index(j), sub, rows, lanes(pos, many)]
        p, a = spot(order, ph, pos, sub), order[ph]
        rows = pl.ds(0, 128) if half is None else pl.ds(64 * half, 64)
        ix, iz = (pl.ds(0, 4) if p[i] is None else pl.ds(p[i], many if i == a else 1) for i in (X, Z))
        if j in SLOTTED:
            return ts_ref.at[SLOTTED.index(j), ix, iz, rows, :]
        cols = pl.ds(0, 512) if p[Y] is None else lanes(p[Y], many if a == Y else 1)
        return t_ref.at[PLAIN.index(j), ix, iz, rows, cols]

    landed = set()

    def run_as(j, ph, s, first):
        if first and j not in landed:
            landed.add(j)
            own_tok[j].wait()
        o = ORDERS[j]
        a, u = o[ph], unit(ph, s)
        p = own[a]
        for half, sign in ((0, 1), (1, -1)) if first else ((1, 1), (0, -1)):
            if first:
                sem = ga.at[j, u, half]
            elif ph < 2:
                sem = gb.at[j, u, half]
            else:
                sem = gc.at[j, u]
            h = slab(o, j, ph, s, p, half)
            remote(h, h, gs.at[j, u], sem, at(a, sign))

    def run_af(j, ph, s, sign):
        o, u = ORDERS[j], unit(ph, s)
        half = 0 if sign > 0 else 1
        ref = slab(o, j, ph, s, place(o[ph], -sign), half)
        wait(ref, ga.at[j, u, half])
        remote(ref, ref, gs.at[j, u], gc.at[j, u], at(o[ph], sign))

    def run_ab(j, ph, s, sign):
        half = 1 if sign > 0 else 0
        wait(slab(ORDERS[j], j, ph, s, place(ORDERS[j][ph], -sign), half), gb.at[j, unit(ph, s), half])

    def run_ad(j, ph, s):
        wait(slab(ORDERS[j], j, ph, s, 0, None, 1 if ph < 2 else 2), gc.at[j, unit(ph, s)])

    def run_lw(j):
        wait(pw.at[j], pw_recv.at[j])
        slot = FIRST.index(j) % 2
        for e in range(2):
            for m, src in ((0, gw), (1, uw)):
                s = pw.at[j, m] if e else src.at[:, :, j]
                pltpu.make_async_copy(s, w_ref.at[slot, pl.ds(2 * e, 2), :, :, pl.ds(m * 384, 384)], w_sem.at[slot]).start()

    def run_dw(j):
        if j == SECOND[0]:
            wait(pd, pd_recv)
        slot = SECOND.index(j) % 2
        for e, src in ((0, dw), (1, pd)):
            for k in range(4):
                pltpu.make_async_copy(
                    src.at[:, :, pl.ds(k * 1024 + j * 128, 128)],
                    d_ref.at[slot, pl.ds(2 * e, 2), :, pl.ds(k * 128, 128)], d_sem.at[slot]).start()

    def table(dst, step, pos):
        return dst.at[pl.ds(pos, 1), pl.ds(z, 1)] if step < 3 else dst.at[:, pl.ds(pos, 1)]

    def send_meta(step, pos, axis, sign):
        for i, (_, dst) in enumerate(tables):
            ref = table(dst, step, pos)
            remote(ref, ref, meta_send.at[i, step], meta_recv.at[i, step], at(axis, sign))

    def wait_meta(step):
        for i, (_, dst) in enumerate(tables):
            wait(table(dst, step, 0), meta_recv.at[i, step])

    def run_ma():
        for c in own_meta:
            c.wait()
        send_meta(0, x, X, 1)
        send_meta(1, x, X, -1)

    def run_mb():
        wait_meta(0)
        wait_meta(1)
        send_meta(2, place(X, -1), X, 1)

    def run_mc():
        wait_meta(2)
        send_meta(3, z, Z, 1)
        send_meta(4, z, Z, -1)

    def run_md():
        wait_meta(3)
        wait_meta(4)
        send_meta(5, place(Z, -1), Z, 1)

    def run_meta():
        wait_meta(5)
        ids = mbi[...].reshape(16, 8, 128)
        probs = mbp[...].reshape(16, 8, 128)
        chip = (x * 4 + z) * 4
        rows, prows = [], []
        for e in (chip + 2 * core, chip + 2 * core + 1, chip + 2 * (1 - core), chip + 2 * (1 - core) + 1):
            hit = ids == e
            rows.append(jnp.sum(jnp.where(hit, 1.0, 0.0), axis=1))
            prows.append(jnp.sum(jnp.where(hit, probs, 0.0), axis=1))
        ind = jnp.concatenate(rows, axis=0)
        pr[...] = jnp.concatenate(prows, axis=0)
        upper = (lax.broadcasted_iota(jnp.int32, (128, 128), 0) < lax.broadcasted_iota(jnp.int32, (128, 128), 1))
        rank = jnp.dot(ind.astype(BF16), jnp.where(upper, 1.0, 0.0).astype(BF16), preferred_element_type=F32)
        odd = (lax.broadcasted_iota(jnp.int32, (64, 128), 0) % 2).astype(F32) * float(CAP)
        rk[...] = jnp.where(ind > 0.5, rank + odd, -1.0)

    def run_sb(q):
        row = lax.broadcasted_iota(jnp.int32, (PAIR, 128), 0).astype(F32)
        blocks = []
        for e in range(4):
            i = e * 16 + 2 * q
            left = jnp.where(row == rk[i:i + 1, :], 1.0, 0.0)
            right = jnp.where(row == rk[i + 1:i + 2, :], 1.0, 0.0)
            weight = jnp.sum(left * pr[i:i + 1, :] + right * pr[i + 1:i + 2, :], axis=1, keepdims=True)
            ps[e, q * PAIR:(q + 1) * PAIR, :] = jnp.broadcast_to(0.5 * weight, (PAIR, 128))
            blocks.append(jnp.concatenate([left, right], axis=1))
        blocks.append(jnp.zeros((256 - 4 * PAIR, 256), F32))
        full = jnp.concatenate(blocks, axis=0)
        s_ref[q] = full[:4 * PAIR].astype(BF16)
        st_ref[q] = full.T.astype(BF16)
        for i in range(2):
            y_ref[i, q, 4 * PAIR:, :] = jnp.zeros((256 - 4 * PAIR, 512), BF16)
        for i in range(len(SLOTTED)):
            ys_ref[i, q, 4 * PAIR:, :] = jnp.zeros((256 - 4 * PAIR, 128), BF16)

    def run_sel(j):
        slotted = j in SLOTTED

        def step(i, carry):
            for k in range(4):
                q = 4 * i + k
                gx, gz = 2 * i + k // 2, slice((k % 2) * 2, (k % 2) * 2 + 2)
                if slotted:
                    t = ts_ref[SLOTTED.index(j), gx, gz].reshape(256, 128)
                else:
                    t = t_ref[PLAIN.index(j), gx, gz].reshape(256, 512)
                r = jnp.dot(s_ref[q], t, preferred_element_type=F32).astype(BF16)
                for e in range(4):
                    rows = pl.ds(pl.multiple_of(q * PAIR, 16), PAIR)
                    if slotted:
                        xs_ref[SLOTTED.index(j), e, rows, lanes(y)] = r[e * PAIR:(e + 1) * PAIR]
                    else:
                        x_ref[PLAIN_TURN[j], e, rows, :] = r[e * PAIR:(e + 1) * PAIR]
            return carry

        lax.fori_loop(0, 2, step, 0)

    def run_gu(j, part):
        slot = FIRST.index(j) % 2
        if part in (None, 0):
            wait(w_ref.at[slot], w_sem.at[slot])

        def step(e, carry):
            rows = xs_ref[SLOTTED.index(j), e] if j in SLOTTED else x_ref[PLAIN_TURN[j], e]
            for n in range(3):
                w = w_ref[slot, e, :, :, n * 256:(n + 1) * 256].reshape(512, 256)
                r = jnp.dot(rows, w, preferred_element_type=F32)
                if j == FIRST[0]:
                    acc[e, :, n * 256:(n + 1) * 256] = r
                else:
                    acc[e, :, n * 256:(n + 1) * 256] += r
            return carry

        lax.fori_loop(0, 4, step, 0) if part is None else step(part, 0)

    def run_hid(e):
        def step(k, carry):
            rows = pl.ds(pl.multiple_of(k * 96, 16), 96)
            w = ps[e, rows, :]
            for n in range(3):
                gate, up = acc[e, rows, n * 128:(n + 1) * 128], acc[e, rows, 384 + n * 128:384 + (n + 1) * 128]
                h = (gate * up * w) * (1.0 + jnp.tanh(0.5 * gate))
                hid[e, rows, n * 128:(n + 1) * 128] = h.astype(BF16)
            return carry

        lax.fori_loop(0, 4, step, 0)

    def run_dn(j, part):
        slot = SECOND.index(j) % 2
        slotted = j in SLOTTED
        if part in (None, 0):
            wait(d_ref.at[slot], d_sem.at[slot])
        if slotted and part in (None, 0):
            for s in range(4):
                wait(slab(ORDERS[j], j, 2, s, 0, None, 3), gs.at[j, unit(2, s)])

        def step(e, carry):
            r = jnp.dot(hid[e], d_ref[slot, e], preferred_element_type=F32).astype(BF16)
            if slotted:
                xs_ref[SLOTTED.index(j), e] = r
            else:
                for q in range(NP):
                    y_ref[BACK_PLAIN.index(j) % 2, q, pl.ds(pl.multiple_of(e * PAIR, 16), PAIR), :] = r[q * PAIR:(q + 1) * PAIR]
            return carry

        lax.fori_loop(0, 4, step, 0) if part is None else step(part, 0)

    def run_cb(j):
        slotted = j in SLOTTED
        for ph, s in ((ph, s) for ph in range(2 if slotted else 3) for s in range(SPLIT[ph])):
            wait(slab(ORDERS[j], j, ph, s, 0, None, 3), gs.at[j, unit(ph, s)])

        def step(i, carry):
            for k in range(4):
                q = 4 * i + k
                gx, gz = 2 * i + k // 2, slice((k % 2) * 2, (k % 2) * 2 + 2)
                rows = ys_ref[SLOTTED.index(j), q] if slotted else y_ref[BACK_PLAIN.index(j) % 2, q]
                r = jnp.dot(st_ref[q], rows, preferred_element_type=F32).astype(BF16)
                if slotted:
                    ts_ref[SLOTTED.index(j), gx, gz] = r.reshape(2, 128, 128)
                else:
                    t_ref[PLAIN.index(j), gx, gz] = r.reshape(2, 128, 512)
            return carry

        lax.fori_loop(0, 2, step, 0)

    def buf(j, ph, s):
        return rb[3 * j + ph].at[s]

    def run_rs(j, ph, s, first):
        o = BACK[j]
        a, u = o[ph], unit(ph, s)
        b = buf(j, ph, s)
        for half, sign in ((0, 1), (1, -1)) if first else ((1, 1), (0, -1)):
            pos = place(a, 2 if first else sign)
            sem = ra.at[j, u, half] if first else rc.at[j, u]
            remote(slab(o, j, ph, s, pos, half), b.at[half if first else 3 - half], rs.at[j, u], sem, at(a, sign))

    def add_into(j, ph, s, pos, half, parts, final):
        b, o = rb[3 * j + ph], BACK[j]
        if j in SLOTTED and ph == 2:
            i = SLOTTED.index(j)
            v = xs_ref[i, s, pl.ds(192 * half, 192), lanes(pos)].astype(F32)
            for k in parts:
                v = v + b[s, k].astype(F32)
            v = v.astype(BF16)
            if final:
                for q in range(4):
                    ys_ref[i, 4 * half + q, s * PAIR:(s + 1) * PAIR, :] = v[q * PAIR:(q + 1) * PAIR]
            else:
                xs_ref[i, s, pl.ds(192 * half, 192), lanes(pos)] = v
            return
        nx, nz, _, cols = half_shape(j, o, ph)
        p = spot(o, ph, pos, s)
        rows = pl.ds(64 * half, 64)

        def step(i, carry):
            ix, iz = i // nz, i % nz
            gx, gz = ix if p[X] is None else p[X], iz if p[Z] is None else p[Z]
            if j in SLOTTED:
                ref, where = ts_ref, (SLOTTED.index(j), gx, gz, rows, slice(None))
            else:
                ref = t_ref
                where = (PLAIN.index(j), gx, gz, rows, slice(None) if p[Y] is None else lanes(p[Y]))
            v = ref[where].astype(F32)
            for k in parts:
                v = v + b[s, k, ix, iz].astype(F32)
            v = v.astype(BF16)
            if final and ph == 0:
                out[rows, j * 128:(j + 1) * 128] = v
            else:
                ref[where] = v
            return carry

        if nx * nz == 1:
            step(0, 0)
        else:
            lax.fori_loop(0, nx * nz, step, 0)

    def run_rf(j, ph, s, sign):
        o, u, b = BACK[j], unit(ph, s), buf(j, ph, s)
        half = 0 if sign > 0 else 1
        wait(b.at[half], ra.at[j, u, half])
        pos = place(o[ph], sign)
        add_into(j, ph, s, pos, half, (half,), False)
        remote(slab(o, j, ph, s, pos, half), b.at[4 + half], rs.at[j, u], rc.at[j, u], at(o[ph], sign))

    def run_rd(j, ph, s):
        wait(buf(j, ph, s).at[pl.ds(2, 4)], rc.at[j, unit(ph, s)])
        p = own[BACK[j][ph]]
        add_into(j, ph, s, p, 0, (3, 4), True)
        add_into(j, ph, s, p, 1, (2, 5), True)

    started = 0
    while SCHEDULE[started][0] in ("AS0", "AS1", "MA"):
        k = SCHEDULE[started]
        run_ma() if k[0] == "MA" else run_as(*k[1:], k[0] == "AS0")
        started += 1
    for j in FIRST:
        remote(gw.at[:, :, j], pw.at[j, 0], pw_send, pw_recv.at[j], partner)
        remote(uw.at[:, :, j], pw.at[j, 1], pw_send, pw_recv.at[j], partner)
    remote(dw, pd, pd_send, pd_recv, partner)

    runs = {
        "AS0": lambda *k: run_as(*k, True), "AS1": lambda *k: run_as(*k, False),
        "AF+": lambda *k: run_af(*k, 1), "AF-": lambda *k: run_af(*k, -1),
        "AB+": lambda *k: run_ab(*k, 1), "AB-": lambda *k: run_ab(*k, -1), "AD": run_ad,
        "LW": run_lw, "DW": run_dw, "SEL": run_sel, "GU": run_gu, "DN": run_dn, "CB": run_cb,
        "RS0": lambda *k: run_rs(*k, True), "RS1": lambda *k: run_rs(*k, False),
        "RF+": lambda *k: run_rf(*k, 1), "RF-": lambda *k: run_rf(*k, -1), "RD": run_rd,
        "MA": run_ma, "MB": run_mb, "MC": run_mc, "MD": run_md, "META": run_meta, "SB": run_sb, "HID": run_hid,
    }
    for task in SCHEDULE[started:]:
        runs[task[0]](*task[1:])

    for j in range(NP):
        for ph in range(3):
            for s in range(SPLIT[ph]):
                wait(slab(BACK[j], j, ph, s, 0, None, 3), rs.at[j, unit(ph, s)])
    for i, (_, dst) in enumerate(tables):
        for step in range(6):
            wait(table(dst, step, 0), meta_send.at[i, step])
    wait(pw, pw_send)
    wait(pd, pd_send)


def body(tokens, expert_ids, gate_prob, gate_weight, up_weight, down_weight):
    gw = gate_weight.reshape(2, 4, NP, 128, 384)
    uw = up_weight.reshape(2, 4, NP, 128, 384)
    hbm = pl.BlockSpec(memory_space=pl.ANY)
    dma = pltpu.SemaphoreType.DMA
    ns = len(SLOTTED)
    scratch = [
        pltpu.VMEM((NP - ns, 4, 4, 128, 512), BF16),
        pltpu.VMEM((ns, 4, 4, 128, 128), BF16),
        pltpu.VMEM((ns, 4, 384, 512), BF16),
        pltpu.VMEM((ns, 8, 256, 128), BF16),
        pltpu.VMEM((2, 4, 4, 128, 768), BF16),
        pltpu.VMEM((2, 4, 384, 512), BF16),
        pltpu.VMEM((2, 4, 384, 512), BF16),
        pltpu.VMEM((4, 384, 768), F32),
        pltpu.VMEM((4, 384, 384), BF16),
        pltpu.VMEM((2, 8, 256, 512), BF16),
        pltpu.VMEM((8, 4 * PAIR, 256), BF16),
        pltpu.VMEM((8, 256, 256), BF16),
        pltpu.VMEM((4, 384, 128), F32),
        pltpu.VMEM((64, 128), F32),
        pltpu.VMEM((64, 128), F32),
        pltpu.VMEM((4, 4, 8, 128), jnp.int32),
        pltpu.VMEM((4, 4, 8, 128), F32),
        dma((NP, 9, 2)), dma((NP, 5, 2)), dma((NP, 9)), dma((NP, 9)),
        dma((NP, 9, 2)), dma((NP, 9)), dma((NP, 9)),
        dma((NP,)), dma((2, 6)), dma((2, 6)), dma((2,)), dma, dma((NP,)), dma, dma, dma((2,)), dma((2,)),
    ] + [
        pltpu.VMEM((SPLIT[ph], 6) + half_shape(j, BACK[j], ph), BF16)
        for j in range(NP) for ph in range(3)
    ]
    return pl.pallas_call(
        kernel,
        name="moe",
        out_shape=(
            jax.ShapeDtypeStruct((128, 1024), BF16),
            jax.ShapeDtypeStruct((NP, 2, 2, 4, 128, 384), BF16),
            jax.ShapeDtypeStruct((2, 384, 4096), BF16),
        ),
        in_specs=[hbm] * 6,
        out_specs=(pl.BlockSpec(memory_space=pltpu.VMEM), hbm, hbm),
        scratch_shapes=scratch,
        compiler_params=pltpu.CompilerParams(collective_id=0, has_side_effects=True, vmem_limit_bytes=67043328),
    )(tokens, expert_ids.T, gate_prob.T, gw, uw, down_weight)[0]


def solution(mesh):
    in_specs = (
        P("ep", "etp"),
        P("ep", None),
        P("ep", None),
        P("ep", None, "etp"),
        P("ep", None, "etp"),
        P("ep", "etp", None),
    )
    return jax.shard_map(body, mesh=mesh, in_specs=in_specs, out_specs=P("ep", "etp"), check_vma=False)
```

```python
import jax
import jax.numpy as jnp
from jax import lax
from jax.experimental import pallas as pl
from jax.experimental.pallas import tpu as pltpu
from jax.sharding import PartitionSpec as P

MESH = pl.DeviceIdType.MESH
F32 = jnp.float32
BF16 = jnp.bfloat16
X, Y, Z = 0, 1, 2
NP = 8
CAP = 24
PAIR = 2 * CAP
SUB = (0, -1, 1, 2)

ORDERS = (
    (Z, Y, X),
    (Z, X, Y),
    (X, Y, Z),
    (X, Y, Z),
    (Z, X, Y),
    (Z, Y, X),
    (Z, X, Y),
    (Y, X, Z),
)
BACK = (
    (X, Y, Z),
    (Z, X, Y),
    (X, Y, Z),
    (Z, Y, X),
    (Z, X, Y),
    (Z, Y, X),
    (Z, X, Y),
    (Y, X, Z),
)
THERE = ((6, 0, 1), (2, 3, 2), (2, 3, 4), (0, 5, 5), (4, 4, 5), (5, 3, 7), (4, 6, 3), (5, 4, 6))
HOME = ((2, 5, 5), (4, 4, 2), (6, 5, 5), (7, 5, 5), (6, 6, 1), (5, 5, 3), (7, 5, 4), (1, 4, 5))
FIRST = (0, 1, 2, 3, 4, 5, 6, 7)
SECOND = (0, 6, 5, 3, 1, 4, 7, 2)
BACKLOG = 2.0

SPLIT = (1, 4, 4)
COST = dict(SEL=0.76, SLOT=0.35, GU=1.9, HID=0.4, DN=1.45, CB=0.88, CBS=0.45, META=0.3, SB=0.12, ADD=0.12)
FAST = 4


def tasks_of(orders, back, first, second):
    t = {}

    def add(name, group, cost, after=(), needs=(), sends=()):
        t[name] = (group, cost, tuple(after), tuple(needs), tuple(sends))

    def size_of(axis, ph):
        return 16384 if ph < 2 else 49152 if axis == Y else 65536

    def phase(tag, axis, j, ph, s, per, before, second=(), up=(), down=(), last=()):
        k = (j, ph, s)
        size = size_of(axis, ph)
        v = 0.06 + per * size / 262144
        s0, s1, fp, fm = (tag + "S0",) + k, (tag + "S1",) + k, (tag + "F+",) + k, (tag + "F-",) + k
        group = (tag, j, ph, s if tag == "A" else 3 - s)
        add(s0, group + (0,), 0.06, before, (), [(axis, 1, size, ("a+", tag) + k), (axis, -1, size, ("a-", tag) + k)])
        add(s1, group + (1,), 0.06, [s0, *second], (), [(axis, 1, size, ("b+", tag) + k), (axis, -1, size, ("b-", tag) + k)])
        add(fp, group + (-1,), v, [s1, *up], [("a+", tag) + k], [(axis, 1, size, ("c+", tag) + k)])
        add(fm, group + (-1,), v, [s1, *down], [("a-", tag) + k], [(axis, -1, size, ("c-", tag) + k)])
        g = group + (-2,)
        if tag == "A" and ph < 2:
            add(("AB+",) + k, g, 0.02, [fp], [("b+", tag) + k])
            add(("AB-",) + k, g, 0.02, [fm], [("b-", tag) + k])
            add(("AD",) + k, g, 0.02, [("AB+",) + k, ("AB-",) + k], [("c+", tag) + k, ("c-", tag) + k])
        else:
            add((tag + "D",) + k, g, 2 * v if per else 0.02, [fp, fm, *last], [(n, tag) + k for n in ("b+", "b-", "c+", "c-")])

    def every(kind, j, ph):
        return [(kind, j, ph, s) for s in range(SPLIT[ph])]

    def parts(split):
        return range(4) if split else (None,)

    def share(kind, j, e):
        fast = j == first[-1] if kind in ("SEL", "GU") else second.index(j) < FAST
        return COST[kind] * (0.75 if fast else 1.0) * (1.0 if e is None else 0.3)

    def split_gu(j):
        return j == first[-1] and orders[j][2] == Y

    def split_dn(j):
        return second.index(j) < 2 and orders[j][2] == Y

    def gu_end(j):
        return ("GU", j, 3 if split_gu(j) else None)

    def dn_end(j):
        return ("DN", j, 3 if split_dn(j) else None)

    sb = [("SB", q) for q in range(NP)]
    plain = [j for j in first if orders[j][2] != Y]
    back_plain = [j for j in second if orders[j][2] != Y]
    for j in range(NP):
        order, slot = orders[j], orders[j][2] == Y
        for ph in range(3):
            for s in range(SPLIT[ph]):
                if ph == 0:
                    before = []
                elif ph == 2 and slot:
                    before = [("SEL", j)]
                elif ph == 2 and s == 0:
                    before = every("AD", j, 0)
                elif SPLIT[ph] == 1:
                    before = every("AD", j, ph - 1)
                else:
                    before = ([], every("AB+", j, ph - 1), every("AB-", j, ph - 1), every("AD", j, ph - 1))[s]
                phase("A", order[ph], j, ph, s, 0, before)
        at = first.index(j)
        turn = [gu_end(first[at - 1])] if at else []
        if slot:
            add(("SEL", j), ("SLOT", j), COST["SLOT"], every("AD", j, 1) + sb)
        else:
            i = plain.index(j)
            add(("SEL", j), ("SEL", j), share("SEL", j, None), every("AD", j, 2) + sb + ([gu_end(plain[i - 2])] if i > 1 else []))
        for e in parts(split_gu(j)):
            here = every("AD", j, 2) if e is None else [("AD", j, 2, e)]
            prev = [("GU", j, e - 1)] if e else turn
            add(("GU", j, e), ("GU", j, e or 0), share("GU", j, e), [("SEL", j)] + (here if slot else []) + prev, [("pw", at)])
        at = second.index(j)
        i = 0 if slot else back_plain.index(j)
        for e in parts(split_dn(j)):
            prev = [("DN", j, e - 1)] if e else []
            if at and split_dn(j) and split_dn(second[at - 1]):
                prev.append(("DN", second[at - 1], e))
            elif at and not split_dn(j):
                prev.append(dn_end(second[at - 1]))
            if at > 1:
                prev.append(dn_end(second[at - 2]))
            if not slot and i > 1:
                prev.append(("CB", back_plain[i - 2]))
            add(("DN", j, e), ("DN", j, e or 0), share("DN", j, e), [("HID", 3 if e is None else e)] + prev, [("pd",)])
        order, add_us = back[j], COST["ADD"]
        if slot:
            add(("CB", j), ("CBS", j), COST["CBS"], every("RD", j, 2))
        else:
            add(("CB", j), ("CB", j), share("CB", j, None), [dn_end(j)])
        for ph in (2, 1, 0):
            for s in range(SPLIT[ph] - 1, -1, -1):
                if ph == 2:
                    phase("R", order[2], j, 2, s, add_us, [(("DN", j, s) if split_dn(j) else dn_end(j)) if slot else ("CB", j)])
                elif ph == 1 and slot:
                    phase("R", order[1], j, 1, s, add_us, [("CB", j)])
                elif SPLIT[ph + 1] == 1:
                    phase("R", order[ph], j, ph, s, add_us, [("RD", j, ph + 1, 0)])
                else:
                    d = [[("RD", j, ph + 1, i)] for i in range(4)]
                    phase("R", order[ph], j, ph, s, add_us, d[3], d[1] + d[2], d[2], d[1], d[0])
    add(("MA",), ("M",), 0.05, (), (), [(X, 1, 8192, ("m0",)), (X, -1, 8192, ("m1",))])
    add(("MB",), ("M",), 0.05, [("MA",)], [("m0",), ("m1",)], [(X, 1, 8192, ("m2",))])
    add(("MC",), ("M",), 0.05, [("MB",)], [("m2",)], [(Z, 1, 32768, ("m3",)), (Z, -1, 32768, ("m4",))])
    add(("MD",), ("M",), 0.05, [("MC",)], [("m3",), ("m4",)], [(Z, 1, 32768, ("m5",))])
    add(("META",), ("META",), COST["META"], [("MD",)], [("m5",)])
    for q in range(NP):
        add(("SB", q), ("SB", q), COST["SB"], [("META",)])
    for e in range(4):
        add(("HID", e), ("HID", e), COST["HID"] / 4, [("GU", first[-1], e) if split_gu(first[-1]) else gu_end(first[-1])])
    return t


def priority(there, home, first, second):
    def rank(g):
        if g[0] == "A":
            return (0, -9 if g[4] == -2 else there[g[1]][g[2]], g[3], g[4])
        if g[0] == "R":
            return (0, home[g[1]][g[2]], g[3], g[4])
        if g[0] == "CBS":
            return (0, home[g[1]][2], 9, 0)
        if g[0] == "M":
            return (0, -8, 0, 0)
        if g[0] in ("META", "SB", "SLOT"):
            return (1, 0, 0, 0)
        if g[0] in ("SEL", "GU") and g[1] != first[-1]:
            return (2, first.index(g[1]), g[0] == "GU", 0)
        if g[0] == "SEL":
            return (2, 49, 0, 0)
        if g[0] in ("GU", "HID"):
            return (2, 50, g[-1], g[0] == "HID")
        if g[0] == "CB":
            return (2, 51, 0, 0)
        return (2, 60 + second.index(g[1]), g[2], 0)

    return rank


def plan(t, rank, backlog, trace=None):
    rate, lat = 46.6e3, 2.9
    arrive = {("pd",): 54.0}
    for j in range(NP):
        arrive[("pw", j)] = 8.5 + 4.5 * j
    ids = {k: i for i, k in enumerate(sorted(t, key=lambda k: tuple(str(v) for v in k)))}
    left = {k: len(v[2]) for k, v in t.items()}
    after = {}
    for k, v in t.items():
        for d in v[2]:
            after.setdefault(d, []).append(k)
    avail = [k for k, c in left.items() if c == 0]
    free, now, out = {}, 0.0, []
    while avail:
        best, later = None, 1e9
        for k in avail:
            group, cost, _, needs, sends = t[k]
            when = 0.0
            for n in needs:
                when = max(when, arrive.get(n, 1e9))
            if not needs:
                for a, d, _, _ in sends:
                    when = max(when, free.get((a, d), 0.0) - backlog)
            if when <= now + 1e-9:
                p = rank(group)
                if best is None or (p, ids[k]) < best[:2]:
                    best = (p, ids[k], k)
            elif when < later:
                later = when
        if best is None:
            now = later
            continue
        k = best[2]
        avail.remove(k)
        _, cost, _, _, sends = t[k]
        now += cost
        for a, d, size, tag in sends:
            begin = max(now, free.get((a, d), 0.0))
            free[(a, d)] = begin + size / rate
            arrive[tag] = begin + size / rate + lat
        out.append(k)
        if trace is not None:
            trace.append((round(now, 1), k))
        for q in after.get(k, ()):
            left[q] -= 1
            if left[q] == 0:
                avail.append(q)
    return out, now


def schedule():
    trace = []
    plan(tasks_of(ORDERS, BACK, FIRST, SECOND), priority(THERE, HOME, FIRST, SECOND), BACKLOG, trace)
    out, early = [], [(14.0, FIRST[0]), (19.0, FIRST[1])]
    for when, k in trace:
        while early and when >= early[0][0]:
            out.append(("LW", early.pop(0)[1]))
        out.append(k)
        if k[0] == "GU" and k[2] in (None, 3):
            i = FIRST.index(k[1]) + 2
            out += [("LW", FIRST[i])] if i < NP else [("DW", SECOND[i - NP])]
        if k[0] == "DN" and k[2] in (None, 3) and SECOND.index(k[1]) + 2 < NP:
            out.append(("DW", SECOND[SECOND.index(k[1]) + 2]))
    return out


SCHEDULE = schedule()
SLOTTED = [j for j in range(NP) if ORDERS[j][2] == Y]
PLAIN = [j for j in range(NP) if ORDERS[j][2] != Y]
PLAIN_TURN = {j: i % 2 for i, j in enumerate(k for k in FIRST if k in PLAIN)}
BACK_PLAIN = [j for j in SECOND if ORDERS[j][2] != Y]


def unit(ph, s):
    return sum(SPLIT[:ph]) + s


def half_shape(j, order, ph):
    if j in SLOTTED and ph == 2:
        return (192, 128)
    full = order[:1] if ph == 2 else ()
    return (4 if X in full else 1, 4 if Z in full else 1, 64, 512 if Y in full else 128)


def kernel(tok, ids_t, prob_t, gw, uw, dw, out, pw, pd, t_ref, ts_ref, xs_ref, ys_ref, w_ref, d_ref, x_ref, acc, hid, y_ref,
           s_ref, st_ref, ps, rk, pr, mbi, mbp, ga, gb, gc, gs, ra, rc, rs, tok_sem, meta_send, meta_recv, meta_own,
           pw_send, pw_recv, pd_send, pd_recv, w_sem, d_sem, *rb):
    ep = lax.axis_index("ep")
    y = lax.axis_index("etp")
    x, z, core = ep // 8, (ep // 2) % 4, ep % 2
    own = (x, y, z)

    def at(axis, delta):
        c = [x, y, z]
        c[axis] = (c[axis] + delta + 4) % 4
        return {"ep": c[X] * 8 + c[Z] * 2 + core, "etp": c[Y]}

    partner = {"ep": x * 8 + z * 2 + (1 - core), "etp": y}
    def lanes(i, n=1):
        return pl.ds(pl.multiple_of(i * 128, 128), 128 * n)

    own_tok = []
    for j in range(NP):
        dst = ts_ref.at[SLOTTED.index(j), x, z] if j in SLOTTED else t_ref.at[PLAIN.index(j), x, z, :, lanes(y)]
        own_tok.append(pltpu.make_async_copy(tok.at[:, pl.ds(j * 128, 128)], dst, tok_sem.at[j]))
    for c in own_tok:
        c.start()
    tables = ((ids_t, mbi), (prob_t, mbp))
    own_meta = [pltpu.make_async_copy(src, dst.at[x, z], meta_own.at[i]) for i, (src, dst) in enumerate(tables)]
    for c in own_meta:
        c.start()

    barrier = pltpu.get_barrier_semaphore()
    greet = [at(a, d) for a in (X, Y, Z) for d in (1, -1)] + [partner]
    for d in greet:
        pl.semaphore_signal(barrier, inc=1, device_id=d, device_id_type=MESH)
    pl.semaphore_wait(barrier, len(greet))

    def remote(src, dst, ssem, rsem, dev):
        pltpu.make_async_remote_copy(src_ref=src, dst_ref=dst, send_sem=ssem, recv_sem=rsem,
                                     device_id=dev, device_id_type=MESH).start()

    def wait(ref, sem):
        pltpu.make_async_copy(ref, ref, sem).wait()

    def place(axis, delta):
        return (own[axis] + delta + 4) % 4

    def spot(order, ph, pos, sub):
        p = list(own)
        if ph == 1:
            p[order[0]] = place(order[0], SUB[sub])
        if ph == 2:
            p[order[0]] = None
            p[order[1]] = place(order[1], SUB[sub])
        p[order[ph]] = pos
        return p

    def slab(order, j, ph, sub, pos, half=None, many=1):
        if j in SLOTTED and ph == 2:
            rows = pl.ds(0, 384) if half is None else pl.ds(192 * half, 192)
            return xs_ref.at[SLOTTED.index(j), sub, rows, lanes(pos, many)]
        p, a = spot(order, ph, pos, sub), order[ph]
        rows = pl.ds(0, 128) if half is None else pl.ds(64 * half, 64)
        ix, iz = (pl.ds(0, 4) if p[i] is None else pl.ds(p[i], many if i == a else 1) for i in (X, Z))
        if j in SLOTTED:
            return ts_ref.at[SLOTTED.index(j), ix, iz, rows, :]
        cols = pl.ds(0, 512) if p[Y] is None else lanes(p[Y], many if a == Y else 1)
        return t_ref.at[PLAIN.index(j), ix, iz, rows, cols]

    landed = set()

    def run_as(j, ph, s, first):
        if first and j not in landed:
            landed.add(j)
            own_tok[j].wait()
        o = ORDERS[j]
        a, u = o[ph], unit(ph, s)
        p = own[a]
        for half, sign in ((0, 1), (1, -1)) if first else ((1, 1), (0, -1)):
            if first:
                sem = ga.at[j, u, half]
            elif ph < 2:
                sem = gb.at[j, u, half]
            else:
                sem = gc.at[j, u]
            h = slab(o, j, ph, s, p, half)
            remote(h, h, gs.at[j, u], sem, at(a, sign))

    def run_af(j, ph, s, sign):
        o, u = ORDERS[j], unit(ph, s)
        half = 0 if sign > 0 else 1
        ref = slab(o, j, ph, s, place(o[ph], -sign), half)
        wait(ref, ga.at[j, u, half])
        remote(ref, ref, gs.at[j, u], gc.at[j, u], at(o[ph], sign))

    def run_ab(j, ph, s, sign):
        half = 1 if sign > 0 else 0
        wait(slab(ORDERS[j], j, ph, s, place(ORDERS[j][ph], -sign), half), gb.at[j, unit(ph, s), half])

    def run_ad(j, ph, s):
        wait(slab(ORDERS[j], j, ph, s, 0, None, 1 if ph < 2 else 2), gc.at[j, unit(ph, s)])

    def run_lw(j):
        wait(pw.at[j], pw_recv.at[j])
        slot = FIRST.index(j) % 2
        for e in range(2):
            for m, src in ((0, gw), (1, uw)):
                s = pw.at[j, m] if e else src.at[:, :, j]
                pltpu.make_async_copy(s, w_ref.at[slot, pl.ds(2 * e, 2), :, :, pl.ds(m * 384, 384)], w_sem.at[slot]).start()

    def run_dw(j):
        if j == SECOND[0]:
            wait(pd, pd_recv)
        slot = SECOND.index(j) % 2
        for e, src in ((0, dw), (1, pd)):
            for k in range(4):
                pltpu.make_async_copy(
                    src.at[:, :, pl.ds(k * 1024 + j * 128, 128)],
                    d_ref.at[slot, pl.ds(2 * e, 2), :, pl.ds(k * 128, 128)], d_sem.at[slot]).start()

    def table(dst, step, pos):
        return dst.at[pl.ds(pos, 1), pl.ds(z, 1)] if step < 3 else dst.at[:, pl.ds(pos, 1)]

    def send_meta(step, pos, axis, sign):
        for i, (_, dst) in enumerate(tables):
            ref = table(dst, step, pos)
            remote(ref, ref, meta_send.at[i, step], meta_recv.at[i, step], at(axis, sign))

    def wait_meta(step):
        for i, (_, dst) in enumerate(tables):
            wait(table(dst, step, 0), meta_recv.at[i, step])

    def run_ma():
        for c in own_meta:
            c.wait()
        send_meta(0, x, X, 1)
        send_meta(1, x, X, -1)

    def run_mb():
        wait_meta(0)
        wait_meta(1)
        send_meta(2, place(X, -1), X, 1)

    def run_mc():
        wait_meta(2)
        send_meta(3, z, Z, 1)
        send_meta(4, z, Z, -1)

    def run_md():
        wait_meta(3)
        wait_meta(4)
        send_meta(5, place(Z, -1), Z, 1)

    def run_meta():
        wait_meta(5)
        ids = mbi[...].reshape(16, 8, 128)
        probs = mbp[...].reshape(16, 8, 128)
        chip = (x * 4 + z) * 4
        rows, prows = [], []
        for e in (chip + 2 * core, chip + 2 * core + 1, chip + 2 * (1 - core), chip + 2 * (1 - core) + 1):
            hit = ids == e
            rows.append(jnp.sum(jnp.where(hit, 1.0, 0.0), axis=1))
            prows.append(jnp.sum(jnp.where(hit, probs, 0.0), axis=1))
        ind = jnp.concatenate(rows, axis=0)
        pr[...] = jnp.concatenate(prows, axis=0)
        upper = (lax.broadcasted_iota(jnp.int32, (128, 128), 0) < lax.broadcasted_iota(jnp.int32, (128, 128), 1))
        rank = jnp.dot(ind.astype(BF16), jnp.where(upper, 1.0, 0.0).astype(BF16), preferred_element_type=F32)
        odd = (lax.broadcasted_iota(jnp.int32, (64, 128), 0) % 2).astype(F32) * float(CAP)
        rk[...] = jnp.where(ind > 0.5, rank + odd, -1.0)

    def run_sb(q):
        row = lax.broadcasted_iota(jnp.int32, (PAIR, 128), 0).astype(F32)
        blocks = []
        for e in range(4):
            i = e * 16 + 2 * q
            left = jnp.where(row == rk[i:i + 1, :], 1.0, 0.0)
            right = jnp.where(row == rk[i + 1:i + 2, :], 1.0, 0.0)
            weight = jnp.sum(left * pr[i:i + 1, :] + right * pr[i + 1:i + 2, :], axis=1, keepdims=True)
            ps[e, q * PAIR:(q + 1) * PAIR, :] = jnp.broadcast_to(0.5 * weight, (PAIR, 128))
            blocks.append(jnp.concatenate([left, right], axis=1))
        blocks.append(jnp.zeros((256 - 4 * PAIR, 256), F32))
        full = jnp.concatenate(blocks, axis=0)
        s_ref[q] = full[:4 * PAIR].astype(BF16)
        st_ref[q] = full.T.astype(BF16)
        for i in range(2):
            y_ref[i, q, 4 * PAIR:, :] = jnp.zeros((256 - 4 * PAIR, 512), BF16)
        for i in range(len(SLOTTED)):
            ys_ref[i, q, 4 * PAIR:, :] = jnp.zeros((256 - 4 * PAIR, 128), BF16)

    def loop(n, step, unrolled):
        if unrolled:
            for i in range(n):
                step(i, 0)
        else:
            lax.fori_loop(0, n, step, 0)

    def fast(j):
        return SECOND.index(j) < FAST

    def run_sel(j):
        slotted = j in SLOTTED

        def step(i, carry):
            for k in range(4):
                q = 4 * i + k
                gx, gz = 2 * i + k // 2, slice((k % 2) * 2, (k % 2) * 2 + 2)
                if slotted:
                    t = ts_ref[SLOTTED.index(j), gx, gz].reshape(256, 128)
                else:
                    t = t_ref[PLAIN.index(j), gx, gz].reshape(256, 512)
                r = jnp.dot(s_ref[q], t, preferred_element_type=F32).astype(BF16)
                for e in range(4):
                    rows = pl.ds(pl.multiple_of(q * PAIR, 16), PAIR)
                    if slotted:
                        xs_ref[SLOTTED.index(j), e, rows, lanes(y)] = r[e * PAIR:(e + 1) * PAIR]
                    else:
                        x_ref[PLAIN_TURN[j], e, rows, :] = r[e * PAIR:(e + 1) * PAIR]
            return carry

        loop(2, step, j == FIRST[-1])

    def run_gu(j, part):
        slot = FIRST.index(j) % 2
        if part in (None, 0):
            wait(w_ref.at[slot], w_sem.at[slot])

        def step(e, carry):
            rows = xs_ref[SLOTTED.index(j), e] if j in SLOTTED else x_ref[PLAIN_TURN[j], e]
            for n in range(3):
                w = w_ref[slot, e, :, :, n * 256:(n + 1) * 256].reshape(512, 256)
                r = jnp.dot(rows, w, preferred_element_type=F32)
                if j == FIRST[0]:
                    acc[e, :, n * 256:(n + 1) * 256] = r
                else:
                    acc[e, :, n * 256:(n + 1) * 256] += r
            return carry

        loop(4, step, j == FIRST[-1]) if part is None else step(part, 0)

    def run_hid(e):
        def step(k, carry):
            rows = pl.ds(pl.multiple_of(k * 96, 16), 96)
            w = ps[e, rows, :]
            for n in range(3):
                gate, up = acc[e, rows, n * 128:(n + 1) * 128], acc[e, rows, 384 + n * 128:384 + (n + 1) * 128]
                h = (gate * up * w) * (1.0 + jnp.tanh(0.5 * gate))
                hid[e, rows, n * 128:(n + 1) * 128] = h.astype(BF16)
            return carry

        loop(4, step, True)

    def run_dn(j, part):
        slot = SECOND.index(j) % 2
        slotted = j in SLOTTED
        if part in (None, 0):
            wait(d_ref.at[slot], d_sem.at[slot])
        if slotted and part in (None, 0):
            for s in range(4):
                wait(slab(ORDERS[j], j, 2, s, 0, None, 3), gs.at[j, unit(2, s)])

        def step(e, carry):
            r = jnp.dot(hid[e], d_ref[slot, e], preferred_element_type=F32).astype(BF16)
            if slotted:
                xs_ref[SLOTTED.index(j), e] = r
            else:
                for q in range(NP):
                    y_ref[BACK_PLAIN.index(j) % 2, q, pl.ds(pl.multiple_of(e * PAIR, 16), PAIR), :] = r[q * PAIR:(q + 1) * PAIR]
            return carry

        loop(4, step, fast(j)) if part is None else step(part, 0)

    def run_cb(j):
        slotted = j in SLOTTED
        for ph, s in ((ph, s) for ph in range(2 if slotted else 3) for s in range(SPLIT[ph])):
            wait(slab(ORDERS[j], j, ph, s, 0, None, 3), gs.at[j, unit(ph, s)])

        def step(i, carry):
            for k in range(4):
                q = 4 * i + k
                gx, gz = 2 * i + k // 2, slice((k % 2) * 2, (k % 2) * 2 + 2)
                rows = ys_ref[SLOTTED.index(j), q] if slotted else y_ref[BACK_PLAIN.index(j) % 2, q]
                r = jnp.dot(st_ref[q], rows, preferred_element_type=F32).astype(BF16)
                if slotted:
                    ts_ref[SLOTTED.index(j), gx, gz] = r.reshape(2, 128, 128)
                else:
                    t_ref[PLAIN.index(j), gx, gz] = r.reshape(2, 128, 512)
            return carry

        loop(2, step, fast(j))

    def buf(j, ph, s):
        return rb[3 * j + ph].at[s]

    def run_rs(j, ph, s, first):
        o = BACK[j]
        a, u = o[ph], unit(ph, s)
        b = buf(j, ph, s)
        for half, sign in ((0, 1), (1, -1)) if first else ((1, 1), (0, -1)):
            pos = place(a, 2 if first else sign)
            sem = ra.at[j, u, half] if first else rc.at[j, u]
            remote(slab(o, j, ph, s, pos, half), b.at[half if first else 3 - half], rs.at[j, u], sem, at(a, sign))

    def add_into(j, ph, s, pos, half, parts, final):
        b, o = rb[3 * j + ph], BACK[j]
        if j in SLOTTED and ph == 2:
            i = SLOTTED.index(j)
            v = xs_ref[i, s, pl.ds(192 * half, 192), lanes(pos)].astype(F32)
            for k in parts:
                v = v + b[s, k].astype(F32)
            v = v.astype(BF16)
            if final:
                for q in range(4):
                    ys_ref[i, 4 * half + q, s * PAIR:(s + 1) * PAIR, :] = v[q * PAIR:(q + 1) * PAIR]
            else:
                xs_ref[i, s, pl.ds(192 * half, 192), lanes(pos)] = v
            return
        nx, nz, _, cols = half_shape(j, o, ph)
        p = spot(o, ph, pos, s)
        rows = pl.ds(64 * half, 64)

        def step(i, carry):
            ix, iz = i // nz, i % nz
            gx, gz = ix if p[X] is None else p[X], iz if p[Z] is None else p[Z]
            if j in SLOTTED:
                ref, where = ts_ref, (SLOTTED.index(j), gx, gz, rows, slice(None))
            else:
                ref = t_ref
                where = (PLAIN.index(j), gx, gz, rows, slice(None) if p[Y] is None else lanes(p[Y]))
            v = ref[where].astype(F32)
            for k in parts:
                v = v + b[s, k, ix, iz].astype(F32)
            v = v.astype(BF16)
            if final and ph == 0:
                out[rows, j * 128:(j + 1) * 128] = v
            else:
                ref[where] = v
            return carry

        if nx * nz == 1:
            step(0, 0)
        else:
            lax.fori_loop(0, nx * nz, step, 0)

    def run_rf(j, ph, s, sign):
        o, u, b = BACK[j], unit(ph, s), buf(j, ph, s)
        half = 0 if sign > 0 else 1
        wait(b.at[half], ra.at[j, u, half])
        pos = place(o[ph], sign)
        add_into(j, ph, s, pos, half, (half,), False)
        remote(slab(o, j, ph, s, pos, half), b.at[4 + half], rs.at[j, u], rc.at[j, u], at(o[ph], sign))

    def run_rd(j, ph, s):
        wait(buf(j, ph, s).at[pl.ds(2, 4)], rc.at[j, unit(ph, s)])
        p = own[BACK[j][ph]]
        add_into(j, ph, s, p, 0, (3, 4), True)
        add_into(j, ph, s, p, 1, (2, 5), True)

    started = 0
    while SCHEDULE[started][0] in ("AS0", "AS1", "MA"):
        k = SCHEDULE[started]
        run_ma() if k[0] == "MA" else run_as(*k[1:], k[0] == "AS0")
        started += 1
    for j in FIRST:
        remote(gw.at[:, :, j], pw.at[j, 0], pw_send, pw_recv.at[j], partner)
        remote(uw.at[:, :, j], pw.at[j, 1], pw_send, pw_recv.at[j], partner)
    remote(dw, pd, pd_send, pd_recv, partner)

    runs = {
        "AS0": lambda *k: run_as(*k, True), "AS1": lambda *k: run_as(*k, False),
        "AF+": lambda *k: run_af(*k, 1), "AF-": lambda *k: run_af(*k, -1),
        "AB+": lambda *k: run_ab(*k, 1), "AB-": lambda *k: run_ab(*k, -1), "AD": run_ad,
        "LW": run_lw, "DW": run_dw, "SEL": run_sel, "GU": run_gu, "DN": run_dn, "CB": run_cb,
        "RS0": lambda *k: run_rs(*k, True), "RS1": lambda *k: run_rs(*k, False),
        "RF+": lambda *k: run_rf(*k, 1), "RF-": lambda *k: run_rf(*k, -1), "RD": run_rd,
        "MA": run_ma, "MB": run_mb, "MC": run_mc, "MD": run_md, "META": run_meta, "SB": run_sb, "HID": run_hid,
    }
    for task in SCHEDULE[started:]:
        runs[task[0]](*task[1:])

    for j in range(NP):
        for ph in range(3):
            for s in range(SPLIT[ph]):
                wait(slab(BACK[j], j, ph, s, 0, None, 3), rs.at[j, unit(ph, s)])
    for i, (_, dst) in enumerate(tables):
        for step in range(6):
            wait(table(dst, step, 0), meta_send.at[i, step])
    wait(pw, pw_send)
    wait(pd, pd_send)


def body(tokens, expert_ids, gate_prob, gate_weight, up_weight, down_weight):
    gw = gate_weight.reshape(2, 4, NP, 128, 384)
    uw = up_weight.reshape(2, 4, NP, 128, 384)
    hbm = pl.BlockSpec(memory_space=pl.ANY)
    dma = pltpu.SemaphoreType.DMA
    ns = len(SLOTTED)
    scratch = [
        pltpu.VMEM((NP - ns, 4, 4, 128, 512), BF16),
        pltpu.VMEM((ns, 4, 4, 128, 128), BF16),
        pltpu.VMEM((ns, 4, 384, 512), BF16),
        pltpu.VMEM((ns, 8, 256, 128), BF16),
        pltpu.VMEM((2, 4, 4, 128, 768), BF16),
        pltpu.VMEM((2, 4, 384, 512), BF16),
        pltpu.VMEM((2, 4, 384, 512), BF16),
        pltpu.VMEM((4, 384, 768), F32),
        pltpu.VMEM((4, 384, 384), BF16),
        pltpu.VMEM((2, 8, 256, 512), BF16),
        pltpu.VMEM((8, 4 * PAIR, 256), BF16),
        pltpu.VMEM((8, 256, 256), BF16),
        pltpu.VMEM((4, 384, 128), F32),
        pltpu.VMEM((64, 128), F32),
        pltpu.VMEM((64, 128), F32),
        pltpu.VMEM((4, 4, 8, 128), jnp.int32),
        pltpu.VMEM((4, 4, 8, 128), F32),
        dma((NP, 9, 2)), dma((NP, 5, 2)), dma((NP, 9)), dma((NP, 9)),
        dma((NP, 9, 2)), dma((NP, 9)), dma((NP, 9)),
        dma((NP,)), dma((2, 6)), dma((2, 6)), dma((2,)), dma, dma((NP,)), dma, dma, dma((2,)), dma((2,)),
    ] + [
        pltpu.VMEM((SPLIT[ph], 6) + half_shape(j, BACK[j], ph), BF16)
        for j in range(NP) for ph in range(3)
    ]
    return pl.pallas_call(
        kernel,
        name="moe",
        out_shape=(
            jax.ShapeDtypeStruct((128, 1024), BF16),
            jax.ShapeDtypeStruct((NP, 2, 2, 4, 128, 384), BF16),
            jax.ShapeDtypeStruct((2, 384, 4096), BF16),
        ),
        in_specs=[hbm] * 6,
        out_specs=(pl.BlockSpec(memory_space=pltpu.VMEM), hbm, hbm),
        scratch_shapes=scratch,
        compiler_params=pltpu.CompilerParams(collective_id=0, has_side_effects=True, vmem_limit_bytes=67043328),
    )(tokens, expert_ids.T, gate_prob.T, gw, uw, down_weight)[0]


def solution(mesh):
    in_specs = (
        P("ep", "etp"),
        P("ep", None),
        P("ep", None),
        P("ep", None, "etp"),
        P("ep", None, "etp"),
        P("ep", "etp", None),
    )
    return jax.shard_map(body, mesh=mesh, in_specs=in_specs, out_specs=P("ep", "etp"), check_vma=False)
```

```python
import jax
import jax.numpy as jnp
from jax import lax
from jax.experimental import pallas as pl
from jax.experimental.pallas import tpu as pltpu
from jax.sharding import PartitionSpec as P

MESH = pl.DeviceIdType.MESH
F32 = jnp.float32
BF16 = jnp.bfloat16
X, Y, Z = 0, 1, 2
NP = 8
CAP = 24
PAIR = 2 * CAP
SUB = (0, -1, 1, 2)

ORDERS = (
    (Z, Y, X),
    (Z, X, Y),
    (X, Y, Z),
    (X, Y, Z),
    (Z, X, Y),
    (Z, Y, X),
    (Z, X, Y),
    (Y, X, Z),
)
BACK = (
    (X, Y, Z),
    (Z, X, Y),
    (X, Y, Z),
    (Z, Y, X),
    (Z, X, Y),
    (Z, Y, X),
    (Z, X, Y),
    (Y, X, Z),
)
THERE = ((6, 0, 1), (2, 3, 2), (2, 3, 4), (0, 5, 5), (4, 4, 5), (5, 3, 7), (4, 6, 3), (5, 4, 6))
HOME = ((2, 5, 5), (4, 4, 2), (6, 5, 5), (7, 5, 5), (6, 6, 1), (5, 5, 3), (7, 5, 4), (1, 4, 5))
FIRST = (0, 1, 2, 3, 4, 5, 6, 7)
SECOND = (0, 6, 5, 3, 1, 4, 7, 2)
BACKLOG = 2.0

SPLIT = (1, 4, 4)
COST = dict(SEL=0.76, SLOT=0.35, GU=1.9, HID=0.4, DN=1.45, CB=0.88, CBS=0.45, META=0.3, SB=0.12, ADD=0.12)
FAST = 4


def tasks_of(orders, back, first, second):
    t = {}

    def add(name, group, cost, after=(), needs=(), sends=()):
        t[name] = (group, cost, tuple(after), tuple(needs), tuple(sends))

    def size_of(axis, ph):
        return 16384 if ph < 2 else 49152 if axis == Y else 65536

    def phase(tag, axis, j, ph, s, per, before, second=(), up=(), down=(), last=()):
        k = (j, ph, s)
        size = size_of(axis, ph)
        v = 0.06 + per * size / 262144
        s0, s1, fp, fm = (tag + "S0",) + k, (tag + "S1",) + k, (tag + "F+",) + k, (tag + "F-",) + k
        group = (tag, j, ph, s if tag == "A" else 3 - s)
        add(s0, group + (0,), 0.06, before, (), [(axis, 1, size, ("a+", tag) + k), (axis, -1, size, ("a-", tag) + k)])
        add(s1, group + (1,), 0.06, [s0, *second], (), [(axis, 1, size, ("b+", tag) + k), (axis, -1, size, ("b-", tag) + k)])
        add(fp, group + (-1,), v, [s1, *up], [("a+", tag) + k], [(axis, 1, size, ("c+", tag) + k)])
        add(fm, group + (-1,), v, [s1, *down], [("a-", tag) + k], [(axis, -1, size, ("c-", tag) + k)])
        g = group + (-2,)
        if tag == "A" and ph < 2:
            add(("AB+",) + k, g, 0.02, [fp], [("b+", tag) + k])
            add(("AB-",) + k, g, 0.02, [fm], [("b-", tag) + k])
            add(("AD",) + k, g, 0.02, [("AB+",) + k, ("AB-",) + k], [("c+", tag) + k, ("c-", tag) + k])
        else:
            add((tag + "D",) + k, g, 2 * v if per else 0.02, [fp, fm, *last], [(n, tag) + k for n in ("b+", "b-", "c+", "c-")])

    def every(kind, j, ph):
        return [(kind, j, ph, s) for s in range(SPLIT[ph])]

    def parts(split):
        return range(4) if split else (None,)

    def share(kind, j, e):
        fast = j == first[-1] if kind in ("SEL", "GU") else second.index(j) < FAST
        return COST[kind] * (0.75 if fast else 1.0) * (1.0 if e is None else 0.3)

    def split_gu(j):
        return j == first[-1] and orders[j][2] == Y

    def split_dn(j):
        return second.index(j) < 2 and orders[j][2] == Y

    def gu_end(j):
        return ("GU", j, 3 if split_gu(j) else None)

    def dn_end(j):
        return ("DN", j, 3 if split_dn(j) else None)

    sb = [("SB", q) for q in range(NP)]
    plain = [j for j in first if orders[j][2] != Y]
    back_plain = [j for j in second if orders[j][2] != Y]
    for j in range(NP):
        order, slot = orders[j], orders[j][2] == Y
        for ph in range(3):
            for s in range(SPLIT[ph]):
                if ph == 0:
                    before = []
                elif ph == 2 and slot:
                    before = [("SEL", j)]
                elif ph == 2 and s == 0:
                    before = every("AD", j, 0)
                elif SPLIT[ph] == 1:
                    before = every("AD", j, ph - 1)
                else:
                    before = ([], every("AB+", j, ph - 1), every("AB-", j, ph - 1), every("AD", j, ph - 1))[s]
                phase("A", order[ph], j, ph, s, 0, before)
        at = first.index(j)
        turn = [gu_end(first[at - 1])] if at else []
        if slot:
            add(("SEL", j), ("SLOT", j), COST["SLOT"], every("AD", j, 1) + sb)
        else:
            i = plain.index(j)
            add(("SEL", j), ("SEL", j), share("SEL", j, None), every("AD", j, 2) + sb + ([gu_end(plain[i - 2])] if i > 1 else []))
        for e in parts(split_gu(j)):
            here = every("AD", j, 2) if e is None else [("AD", j, 2, e)]
            prev = [("GU", j, e - 1)] if e else turn
            add(("GU", j, e), ("GU", j, e or 0), share("GU", j, e), [("SEL", j)] + (here if slot else []) + prev, [("pw", at)])
        at = second.index(j)
        i = 0 if slot else back_plain.index(j)
        for e in parts(split_dn(j)):
            prev = [("DN", j, e - 1)] if e else []
            if at and split_dn(j) and split_dn(second[at - 1]):
                prev.append(("DN", second[at - 1], e))
            elif at and not split_dn(j):
                prev.append(dn_end(second[at - 1]))
            if at > 1:
                prev.append(dn_end(second[at - 2]))
            if not slot and i > 1:
                prev.append(("CB", back_plain[i - 2]))
            add(("DN", j, e), ("DN", j, e or 0), share("DN", j, e), [("HID", 3 if e is None else e)] + prev, [("pd",)])
        order, add_us = back[j], COST["ADD"]
        if slot:
            add(("CB", j), ("CBS", j), COST["CBS"], every("RD", j, 2))
        else:
            add(("CB", j), ("CB", j), share("CB", j, None), [dn_end(j)])
        for ph in (2, 1, 0):
            for s in range(SPLIT[ph] - 1, -1, -1):
                if ph == 2:
                    phase("R", order[2], j, 2, s, add_us, [(("DN", j, s) if split_dn(j) else dn_end(j)) if slot else ("CB", j)])
                elif ph == 1 and slot:
                    phase("R", order[1], j, 1, s, add_us, [("CB", j)])
                elif SPLIT[ph + 1] == 1:
                    phase("R", order[ph], j, ph, s, add_us, [("RD", j, ph + 1, 0)])
                else:
                    d = [[("RD", j, ph + 1, i)] for i in range(4)]
                    phase("R", order[ph], j, ph, s, add_us, d[3], d[1] + d[2], d[2], d[1], d[0])
    add(("MA",), ("M",), 0.05, (), (), [(X, 1, 8192, ("m0",)), (X, -1, 8192, ("m1",))])
    add(("MB",), ("M",), 0.05, [("MA",)], [("m0",), ("m1",)], [(X, 1, 8192, ("m2",))])
    add(("MC",), ("M",), 0.05, [("MB",)], [("m2",)], [(Z, 1, 32768, ("m3",)), (Z, -1, 32768, ("m4",))])
    add(("MD",), ("M",), 0.05, [("MC",)], [("m3",), ("m4",)], [(Z, 1, 32768, ("m5",))])
    add(("META",), ("META",), COST["META"], [("MD",)], [("m5",)])
    for q in range(NP):
        add(("SB", q), ("SB", q), COST["SB"], [("META",)])
    for e in range(4):
        add(("HID", e), ("HID", e), COST["HID"] / 4, [("GU", first[-1], e) if split_gu(first[-1]) else gu_end(first[-1])])
    return t


def priority(there, home, first, second):
    def rank(g):
        if g[0] == "A":
            return (0, -9 if g[4] == -2 else there[g[1]][g[2]], g[3], g[4])
        if g[0] == "R":
            return (0, home[g[1]][g[2]], g[3], g[4])
        if g[0] == "CBS":
            return (0, home[g[1]][2], 9, 0)
        if g[0] == "M":
            return (0, -8, 0, 0)
        if g[0] in ("META", "SB", "SLOT"):
            return (1, 0, 0, 0)
        if g[0] in ("SEL", "GU") and g[1] != first[-1]:
            return (2, first.index(g[1]), g[0] == "GU", 0)
        if g[0] == "SEL":
            return (2, 49, 0, 0)
        if g[0] in ("GU", "HID"):
            return (2, 50, g[-1], g[0] == "HID")
        if g[0] == "CB":
            return (2, 51, 0, 0)
        return (2, 60 + second.index(g[1]), g[2], 0)

    return rank


def plan(t, rank, backlog, trace=None):
    rate, lat = 46.6e3, 2.9
    arrive = {("pd",): 54.0}
    for j in range(NP):
        arrive[("pw", j)] = 8.5 + 4.5 * j
    ids = {k: i for i, k in enumerate(sorted(t, key=lambda k: tuple(str(v) for v in k)))}
    left = {k: len(v[2]) for k, v in t.items()}
    after = {}
    for k, v in t.items():
        for d in v[2]:
            after.setdefault(d, []).append(k)
    avail = [k for k, c in left.items() if c == 0]
    free, now, out = {}, 0.0, []
    while avail:
        best, later = None, 1e9
        for k in avail:
            group, cost, _, needs, sends = t[k]
            when = 0.0
            for n in needs:
                when = max(when, arrive.get(n, 1e9))
            if not needs:
                for a, d, _, _ in sends:
                    when = max(when, free.get((a, d), 0.0) - backlog)
            if when <= now + 1e-9:
                p = rank(group)
                if best is None or (p, ids[k]) < best[:2]:
                    best = (p, ids[k], k)
            elif when < later:
                later = when
        if best is None:
            now = later
            continue
        k = best[2]
        avail.remove(k)
        _, cost, _, _, sends = t[k]
        now += cost
        for a, d, size, tag in sends:
            begin = max(now, free.get((a, d), 0.0))
            free[(a, d)] = begin + size / rate
            arrive[tag] = begin + size / rate + lat
        out.append(k)
        if trace is not None:
            trace.append((round(now, 1), k))
        for q in after.get(k, ()):
            left[q] -= 1
            if left[q] == 0:
                avail.append(q)
    return out, now


def schedule():
    trace = []
    plan(tasks_of(ORDERS, BACK, FIRST, SECOND), priority(THERE, HOME, FIRST, SECOND), BACKLOG, trace)
    out, early = [], [(14.0, FIRST[0]), (19.0, FIRST[1])]
    for when, k in trace:
        while early and when >= early[0][0]:
            out.append(("LW", early.pop(0)[1]))
        out.append(k)
        if k[0] == "GU" and k[2] in (None, 3):
            i = FIRST.index(k[1]) + 2
            out += [("LW", FIRST[i])] if i < NP else [("DW", SECOND[i - NP])]
        if k[0] == "DN" and k[2] in (None, 3) and SECOND.index(k[1]) + 2 < NP:
            out.append(("DW", SECOND[SECOND.index(k[1]) + 2]))
    return out


SCHEDULE = schedule()
SLOTTED = [j for j in range(NP) if ORDERS[j][2] == Y]
PLAIN = [j for j in range(NP) if ORDERS[j][2] != Y]
PLAIN_TURN = {j: i % 2 for i, j in enumerate(k for k in FIRST if k in PLAIN)}
BACK_PLAIN = [j for j in SECOND if ORDERS[j][2] != Y]


def unit(ph, s):
    return sum(SPLIT[:ph]) + s


def half_shape(j, order, ph):
    if j in SLOTTED and ph == 2:
        return (192, 128)
    full = order[:1] if ph == 2 else ()
    return (4 if X in full else 1, 4 if Z in full else 1, 64, 512 if Y in full else 128)


def kernel(tok, ids_t, prob_t, gw, uw, dw, result, pw, pd, out, out_sem, t_ref, ts_ref, xs_ref, ys_ref, w_ref, d_ref, x_ref, acc, hid, y_ref,
           s_ref, st_ref, ps, rk, pr, mbi, mbp, ga, gb, gc, gs, ra, rc, rs, tok_sem, meta_send, meta_recv, meta_own,
           pw_send, pw_recv, pd_send, pd_recv, w_sem, d_sem, *rb):
    ep = lax.axis_index("ep")
    y = lax.axis_index("etp")
    x, z, core = ep // 8, (ep // 2) % 4, ep % 2
    own = (x, y, z)

    def at(axis, delta):
        c = [x, y, z]
        c[axis] = (c[axis] + delta + 4) % 4
        return {"ep": c[X] * 8 + c[Z] * 2 + core, "etp": c[Y]}

    partner = {"ep": x * 8 + z * 2 + (1 - core), "etp": y}
    def lanes(i, n=1):
        return pl.ds(pl.multiple_of(i * 128, 128), 128 * n)

    own_tok = []
    for j in range(NP):
        dst = ts_ref.at[SLOTTED.index(j), x, z] if j in SLOTTED else t_ref.at[PLAIN.index(j), x, z, :, lanes(y)]
        own_tok.append(pltpu.make_async_copy(tok.at[:, pl.ds(j * 128, 128)], dst, tok_sem.at[j]))
    for c in own_tok:
        c.start()
    tables = ((ids_t, mbi), (prob_t, mbp))
    own_meta = [pltpu.make_async_copy(src, dst.at[x, z], meta_own.at[i]) for i, (src, dst) in enumerate(tables)]
    for c in own_meta:
        c.start()

    barrier = pltpu.get_barrier_semaphore()
    greet = [at(a, d) for a in (X, Y, Z) for d in (1, -1)] + [partner]
    for d in greet:
        pl.semaphore_signal(barrier, inc=1, device_id=d, device_id_type=MESH)
    pl.semaphore_wait(barrier, len(greet))

    def remote(src, dst, ssem, rsem, dev):
        pltpu.make_async_remote_copy(src_ref=src, dst_ref=dst, send_sem=ssem, recv_sem=rsem,
                                     device_id=dev, device_id_type=MESH).start()

    def wait(ref, sem):
        pltpu.make_async_copy(ref, ref, sem).wait()

    def place(axis, delta):
        return (own[axis] + delta + 4) % 4

    def spot(order, ph, pos, sub):
        p = list(own)
        if ph == 1:
            p[order[0]] = place(order[0], SUB[sub])
        if ph == 2:
            p[order[0]] = None
            p[order[1]] = place(order[1], SUB[sub])
        p[order[ph]] = pos
        return p

    def slab(order, j, ph, sub, pos, half=None, many=1):
        if j in SLOTTED and ph == 2:
            rows = pl.ds(0, 384) if half is None else pl.ds(192 * half, 192)
            return xs_ref.at[SLOTTED.index(j), sub, rows, lanes(pos, many)]
        p, a = spot(order, ph, pos, sub), order[ph]
        rows = pl.ds(0, 128) if half is None else pl.ds(64 * half, 64)
        ix, iz = (pl.ds(0, 4) if p[i] is None else pl.ds(p[i], many if i == a else 1) for i in (X, Z))
        if j in SLOTTED:
            return ts_ref.at[SLOTTED.index(j), ix, iz, rows, :]
        cols = pl.ds(0, 512) if p[Y] is None else lanes(p[Y], many if a == Y else 1)
        return t_ref.at[PLAIN.index(j), ix, iz, rows, cols]

    landed = set()

    def run_as(j, ph, s, first):
        if first and j not in landed:
            landed.add(j)
            own_tok[j].wait()
        o = ORDERS[j]
        a, u = o[ph], unit(ph, s)
        p = own[a]
        for half, sign in ((0, 1), (1, -1)) if first else ((1, 1), (0, -1)):
            if first:
                sem = ga.at[j, u, half]
            elif ph < 2:
                sem = gb.at[j, u, half]
            else:
                sem = gc.at[j, u]
            h = slab(o, j, ph, s, p, half)
            remote(h, h, gs.at[j, u], sem, at(a, sign))

    def run_af(j, ph, s, sign):
        o, u = ORDERS[j], unit(ph, s)
        half = 0 if sign > 0 else 1
        ref = slab(o, j, ph, s, place(o[ph], -sign), half)
        wait(ref, ga.at[j, u, half])
        remote(ref, ref, gs.at[j, u], gc.at[j, u], at(o[ph], sign))

    def run_ab(j, ph, s, sign):
        half = 1 if sign > 0 else 0
        wait(slab(ORDERS[j], j, ph, s, place(ORDERS[j][ph], -sign), half), gb.at[j, unit(ph, s), half])

    def run_ad(j, ph, s):
        wait(slab(ORDERS[j], j, ph, s, 0, None, 1 if ph < 2 else 2), gc.at[j, unit(ph, s)])

    def run_lw(j):
        wait(pw.at[j], pw_recv.at[j])
        slot = FIRST.index(j) % 2
        for e in range(2):
            for m, src in ((0, gw), (1, uw)):
                s = pw.at[j, m] if e else src.at[:, :, j]
                pltpu.make_async_copy(s, w_ref.at[slot, pl.ds(2 * e, 2), :, :, pl.ds(m * 384, 384)], w_sem.at[slot]).start()

    def run_dw(j):
        if j == SECOND[0]:
            wait(pd, pd_recv)
        slot = SECOND.index(j) % 2
        for e, src in ((0, dw), (1, pd)):
            for k in range(4):
                pltpu.make_async_copy(
                    src.at[:, :, pl.ds(k * 1024 + j * 128, 128)],
                    d_ref.at[slot, pl.ds(2 * e, 2), :, pl.ds(k * 128, 128)], d_sem.at[slot]).start()

    def table(dst, step, pos):
        return dst.at[pl.ds(pos, 1), pl.ds(z, 1)] if step < 3 else dst.at[:, pl.ds(pos, 1)]

    def send_meta(step, pos, axis, sign):
        for i, (_, dst) in enumerate(tables):
            ref = table(dst, step, pos)
            remote(ref, ref, meta_send.at[i, step], meta_recv.at[i, step], at(axis, sign))

    def wait_meta(step):
        for i, (_, dst) in enumerate(tables):
            wait(table(dst, step, 0), meta_recv.at[i, step])

    def run_ma():
        for c in own_meta:
            c.wait()
        send_meta(0, x, X, 1)
        send_meta(1, x, X, -1)

    def run_mb():
        wait_meta(0)
        wait_meta(1)
        send_meta(2, place(X, -1), X, 1)

    def run_mc():
        wait_meta(2)
        send_meta(3, z, Z, 1)
        send_meta(4, z, Z, -1)

    def run_md():
        wait_meta(3)
        wait_meta(4)
        send_meta(5, place(Z, -1), Z, 1)

    def run_meta():
        wait_meta(5)
        ids = mbi[...].reshape(16, 8, 128)
        probs = mbp[...].reshape(16, 8, 128)
        chip = (x * 4 + z) * 4
        rows, prows = [], []
        for e in (chip + 2 * core, chip + 2 * core + 1, chip + 2 * (1 - core), chip + 2 * (1 - core) + 1):
            hit = ids == e
            rows.append(jnp.sum(jnp.where(hit, 1.0, 0.0), axis=1))
            prows.append(jnp.sum(jnp.where(hit, probs, 0.0), axis=1))
        ind = jnp.concatenate(rows, axis=0)
        pr[...] = jnp.concatenate(prows, axis=0)
        upper = (lax.broadcasted_iota(jnp.int32, (128, 128), 0) < lax.broadcasted_iota(jnp.int32, (128, 128), 1))
        rank = jnp.dot(ind.astype(BF16), jnp.where(upper, 1.0, 0.0).astype(BF16), preferred_element_type=F32)
        odd = (lax.broadcasted_iota(jnp.int32, (64, 128), 0) % 2).astype(F32) * float(CAP)
        rk[...] = jnp.where(ind > 0.5, rank + odd, -1.0)

    def run_sb(q):
        row = lax.broadcasted_iota(jnp.int32, (PAIR, 128), 0).astype(F32)
        blocks = []
        for e in range(4):
            i = e * 16 + 2 * q
            left = jnp.where(row == rk[i:i + 1, :], 1.0, 0.0)
            right = jnp.where(row == rk[i + 1:i + 2, :], 1.0, 0.0)
            weight = jnp.sum(left * pr[i:i + 1, :] + right * pr[i + 1:i + 2, :], axis=1, keepdims=True)
            ps[e, q * PAIR:(q + 1) * PAIR, :] = jnp.broadcast_to(0.5 * weight, (PAIR, 128))
            blocks.append(jnp.concatenate([left, right], axis=1))
        blocks.append(jnp.zeros((256 - 4 * PAIR, 256), F32))
        full = jnp.concatenate(blocks, axis=0)
        s_ref[q] = full[:4 * PAIR].astype(BF16)
        st_ref[q] = full.T.astype(BF16)
        for i in range(2):
            y_ref[i, q, 4 * PAIR:, :] = jnp.zeros((256 - 4 * PAIR, 512), BF16)
        for i in range(len(SLOTTED)):
            ys_ref[i, q, 4 * PAIR:, :] = jnp.zeros((256 - 4 * PAIR, 128), BF16)

    def loop(n, step, unrolled):
        if unrolled:
            for i in range(n):
                step(i, 0)
        else:
            lax.fori_loop(0, n, step, 0)

    def fast(j):
        return SECOND.index(j) < FAST

    def run_sel(j):
        slotted = j in SLOTTED

        def step(i, carry):
            for k in range(4):
                q = 4 * i + k
                gx, gz = 2 * i + k // 2, slice((k % 2) * 2, (k % 2) * 2 + 2)
                if slotted:
                    t = ts_ref[SLOTTED.index(j), gx, gz].reshape(256, 128)
                else:
                    t = t_ref[PLAIN.index(j), gx, gz].reshape(256, 512)
                r = jnp.dot(s_ref[q], t, preferred_element_type=F32).astype(BF16)
                for e in range(4):
                    rows = pl.ds(pl.multiple_of(q * PAIR, 16), PAIR)
                    if slotted:
                        xs_ref[SLOTTED.index(j), e, rows, lanes(y)] = r[e * PAIR:(e + 1) * PAIR]
                    else:
                        x_ref[PLAIN_TURN[j], e, rows, :] = r[e * PAIR:(e + 1) * PAIR]
            return carry

        loop(2, step, j == FIRST[-1])

    def run_gu(j, part):
        slot = FIRST.index(j) % 2
        if part in (None, 0):
            wait(w_ref.at[slot], w_sem.at[slot])

        def step(e, carry):
            rows = xs_ref[SLOTTED.index(j), e] if j in SLOTTED else x_ref[PLAIN_TURN[j], e]
            for n in range(3):
                w = w_ref[slot, e, :, :, n * 256:(n + 1) * 256].reshape(512, 256)
                r = jnp.dot(rows, w, preferred_element_type=F32)
                if j == FIRST[0]:
                    acc[e, :, n * 256:(n + 1) * 256] = r
                else:
                    acc[e, :, n * 256:(n + 1) * 256] += r
            return carry

        loop(4, step, j == FIRST[-1]) if part is None else step(part, 0)

    def run_hid(e):
        def step(k, carry):
            rows = pl.ds(pl.multiple_of(k * 96, 16), 96)
            w = ps[e, rows, :]
            for n in range(3):
                gate, up = acc[e, rows, n * 128:(n + 1) * 128], acc[e, rows, 384 + n * 128:384 + (n + 1) * 128]
                h = (gate * up * w) * (1.0 + jnp.tanh(0.5 * gate))
                hid[e, rows, n * 128:(n + 1) * 128] = h.astype(BF16)
            return carry

        loop(4, step, True)

    def run_dn(j, part):
        slot = SECOND.index(j) % 2
        slotted = j in SLOTTED
        if part in (None, 0):
            wait(d_ref.at[slot], d_sem.at[slot])
        if slotted and part in (None, 0):
            for s in range(4):
                wait(slab(ORDERS[j], j, 2, s, 0, None, 3), gs.at[j, unit(2, s)])

        def step(e, carry):
            r = jnp.dot(hid[e], d_ref[slot, e], preferred_element_type=F32).astype(BF16)
            if slotted:
                xs_ref[SLOTTED.index(j), e] = r
            else:
                for q in range(NP):
                    y_ref[BACK_PLAIN.index(j) % 2, q, pl.ds(pl.multiple_of(e * PAIR, 16), PAIR), :] = r[q * PAIR:(q + 1) * PAIR]
            return carry

        loop(4, step, fast(j)) if part is None else step(part, 0)

    def run_cb(j):
        slotted = j in SLOTTED
        for ph, s in ((ph, s) for ph in range(2 if slotted else 3) for s in range(SPLIT[ph])):
            wait(slab(ORDERS[j], j, ph, s, 0, None, 3), gs.at[j, unit(ph, s)])

        def step(i, carry):
            for k in range(4):
                q = 4 * i + k
                gx, gz = 2 * i + k // 2, slice((k % 2) * 2, (k % 2) * 2 + 2)
                rows = ys_ref[SLOTTED.index(j), q] if slotted else y_ref[BACK_PLAIN.index(j) % 2, q]
                r = jnp.dot(st_ref[q], rows, preferred_element_type=F32).astype(BF16)
                if slotted:
                    ts_ref[SLOTTED.index(j), gx, gz] = r.reshape(2, 128, 128)
                else:
                    t_ref[PLAIN.index(j), gx, gz] = r.reshape(2, 128, 512)
            return carry

        loop(2, step, fast(j))

    def buf(j, ph, s):
        return rb[3 * j + ph].at[s]

    def run_rs(j, ph, s, first):
        o = BACK[j]
        a, u = o[ph], unit(ph, s)
        b = buf(j, ph, s)
        for half, sign in ((0, 1), (1, -1)) if first else ((1, 1), (0, -1)):
            pos = place(a, 2 if first else sign)
            sem = ra.at[j, u, half] if first else rc.at[j, u]
            remote(slab(o, j, ph, s, pos, half), b.at[half if first else 3 - half], rs.at[j, u], sem, at(a, sign))

    def add_into(j, ph, s, pos, half, parts, final):
        b, o = rb[3 * j + ph], BACK[j]
        if j in SLOTTED and ph == 2:
            i = SLOTTED.index(j)
            v = xs_ref[i, s, pl.ds(192 * half, 192), lanes(pos)].astype(F32)
            for k in parts:
                v = v + b[s, k].astype(F32)
            v = v.astype(BF16)
            if final:
                for q in range(4):
                    ys_ref[i, 4 * half + q, s * PAIR:(s + 1) * PAIR, :] = v[q * PAIR:(q + 1) * PAIR]
            else:
                xs_ref[i, s, pl.ds(192 * half, 192), lanes(pos)] = v
            return
        nx, nz, _, cols = half_shape(j, o, ph)
        p = spot(o, ph, pos, s)
        rows = pl.ds(64 * half, 64)

        def step(i, carry):
            ix, iz = i // nz, i % nz
            gx, gz = ix if p[X] is None else p[X], iz if p[Z] is None else p[Z]
            if j in SLOTTED:
                ref, where = ts_ref, (SLOTTED.index(j), gx, gz, rows, slice(None))
            else:
                ref = t_ref
                where = (PLAIN.index(j), gx, gz, rows, slice(None) if p[Y] is None else lanes(p[Y]))
            v = ref[where].astype(F32)
            for k in parts:
                v = v + b[s, k, ix, iz].astype(F32)
            v = v.astype(BF16)
            if final and ph == 0:
                out[rows, j * 128:(j + 1) * 128] = v
            else:
                ref[where] = v
            return carry

        if nx * nz == 1:
            step(0, 0)
        else:
            lax.fori_loop(0, nx * nz, step, 0)

    def run_rf(j, ph, s, sign):
        o, u, b = BACK[j], unit(ph, s), buf(j, ph, s)
        half = 0 if sign > 0 else 1
        wait(b.at[half], ra.at[j, u, half])
        pos = place(o[ph], sign)
        add_into(j, ph, s, pos, half, (half,), False)
        remote(slab(o, j, ph, s, pos, half), b.at[4 + half], rs.at[j, u], rc.at[j, u], at(o[ph], sign))

    def write_back(j):
        cols = pl.ds(j * 128, 128)
        return pltpu.make_async_copy(out.at[:, cols], result.at[:, cols], out_sem.at[j])

    def run_rd(j, ph, s):
        wait(buf(j, ph, s).at[pl.ds(2, 4)], rc.at[j, unit(ph, s)])
        p = own[BACK[j][ph]]
        add_into(j, ph, s, p, 0, (3, 4), True)
        add_into(j, ph, s, p, 1, (2, 5), True)
        if ph == 0:
            write_back(j).start()

    started = 0
    while SCHEDULE[started][0] in ("AS0", "AS1", "MA"):
        k = SCHEDULE[started]
        run_ma() if k[0] == "MA" else run_as(*k[1:], k[0] == "AS0")
        started += 1
    for j in FIRST:
        remote(gw.at[:, :, j], pw.at[j, 0], pw_send, pw_recv.at[j], partner)
        remote(uw.at[:, :, j], pw.at[j, 1], pw_send, pw_recv.at[j], partner)
    remote(dw, pd, pd_send, pd_recv, partner)

    runs = {
        "AS0": lambda *k: run_as(*k, True), "AS1": lambda *k: run_as(*k, False),
        "AF+": lambda *k: run_af(*k, 1), "AF-": lambda *k: run_af(*k, -1),
        "AB+": lambda *k: run_ab(*k, 1), "AB-": lambda *k: run_ab(*k, -1), "AD": run_ad,
        "LW": run_lw, "DW": run_dw, "SEL": run_sel, "GU": run_gu, "DN": run_dn, "CB": run_cb,
        "RS0": lambda *k: run_rs(*k, True), "RS1": lambda *k: run_rs(*k, False),
        "RF+": lambda *k: run_rf(*k, 1), "RF-": lambda *k: run_rf(*k, -1), "RD": run_rd,
        "MA": run_ma, "MB": run_mb, "MC": run_mc, "MD": run_md, "META": run_meta, "SB": run_sb, "HID": run_hid,
    }
    for task in SCHEDULE[started:]:
        runs[task[0]](*task[1:])

    for j in range(NP):
        for ph in range(3):
            for s in range(SPLIT[ph]):
                wait(slab(BACK[j], j, ph, s, 0, None, 3), rs.at[j, unit(ph, s)])
    for i, (_, dst) in enumerate(tables):
        for step in range(6):
            wait(table(dst, step, 0), meta_send.at[i, step])
    for j in range(NP):
        write_back(j).wait()
    wait(pw, pw_send)
    wait(pd, pd_send)


def body(tokens, expert_ids, gate_prob, gate_weight, up_weight, down_weight):
    gw = gate_weight.reshape(2, 4, NP, 128, 384)
    uw = up_weight.reshape(2, 4, NP, 128, 384)
    hbm = pl.BlockSpec(memory_space=pl.ANY)
    dma = pltpu.SemaphoreType.DMA
    ns = len(SLOTTED)
    scratch = [
        pltpu.VMEM((128, 1024), BF16),
        dma((NP,)),
        pltpu.VMEM((NP - ns, 4, 4, 128, 512), BF16),
        pltpu.VMEM((ns, 4, 4, 128, 128), BF16),
        pltpu.VMEM((ns, 4, 384, 512), BF16),
        pltpu.VMEM((ns, 8, 256, 128), BF16),
        pltpu.VMEM((2, 4, 4, 128, 768), BF16),
        pltpu.VMEM((2, 4, 384, 512), BF16),
        pltpu.VMEM((2, 4, 384, 512), BF16),
        pltpu.VMEM((4, 384, 768), F32),
        pltpu.VMEM((4, 384, 384), BF16),
        pltpu.VMEM((2, 8, 256, 512), BF16),
        pltpu.VMEM((8, 4 * PAIR, 256), BF16),
        pltpu.VMEM((8, 256, 256), BF16),
        pltpu.VMEM((4, 384, 128), F32),
        pltpu.VMEM((64, 128), F32),
        pltpu.VMEM((64, 128), F32),
        pltpu.VMEM((4, 4, 8, 128), jnp.int32),
        pltpu.VMEM((4, 4, 8, 128), F32),
        dma((NP, 9, 2)), dma((NP, 5, 2)), dma((NP, 9)), dma((NP, 9)),
        dma((NP, 9, 2)), dma((NP, 9)), dma((NP, 9)),
        dma((NP,)), dma((2, 6)), dma((2, 6)), dma((2,)), dma, dma((NP,)), dma, dma, dma((2,)), dma((2,)),
    ] + [
        pltpu.VMEM((SPLIT[ph], 6) + half_shape(j, BACK[j], ph), BF16)
        for j in range(NP) for ph in range(3)
    ]
    return pl.pallas_call(
        kernel,
        name="moe",
        out_shape=(
            jax.ShapeDtypeStruct((128, 1024), BF16),
            jax.ShapeDtypeStruct((NP, 2, 2, 4, 128, 384), BF16),
            jax.ShapeDtypeStruct((2, 384, 4096), BF16),
        ),
        in_specs=[hbm] * 6,
        out_specs=(hbm, hbm, hbm),
        scratch_shapes=scratch,
        compiler_params=pltpu.CompilerParams(collective_id=0, has_side_effects=True, vmem_limit_bytes=67043328),
    )(tokens, expert_ids.T, gate_prob.T, gw, uw, down_weight)[0]


def solution(mesh):
    in_specs = (
        P("ep", "etp"),
        P("ep", None),
        P("ep", None),
        P("ep", None, "etp"),
        P("ep", None, "etp"),
        P("ep", "etp", None),
    )
    return jax.shard_map(body, mesh=mesh, in_specs=in_specs, out_specs=P("ep", "etp"), check_vma=False)
```
